32 devices in a mesh: frag: 8 (over z, y), blk: 4 (over x, core).
Axes of the slice: x: 2, y: 2, z: 4, core: 2. Of those that a mesh axis runs over, the one named last changes fastest.
Arguments:
- amps: float32 [8, 128, 8, 128], P('frag', 'blk'), may hold values from -1.5 to 1.5
- exch: float32 [8, 128, 8, 128], P('frag', 'blk'), may hold values from -4 to 4
- factors: bfloat16 [8, 384, 128, 128], P('frag', 'blk'), may hold values from -0.109375 to 0.109375
- occupied_pair_ladder: float32 [8, 8, 8], P('frag'), may hold values from -1 to 1
- virtual_fock_block: float32 [8, 128, 128], P('frag'), may hold values from -0.1875 to 0.1875
- virtual_orbital_energy: float32 [8, 128], P('frag'), may hold values from 1 to 3
- pair_energy: float32 [8, 8], P('frag'), may hold values from -1.5 to -0.5
- energy_weight: int32 [8, 8], P('frag'), may hold values from 0 to 2
- export_rows: int32 [8, 2, 2], P('frag'), may hold values from 2 to 5, as said below
Outputs:
- new_amps: float32 [8, 128, 8, 128], P('frag', 'blk')
- res_norms: float32 [8, 2], P('frag')
- energy: float32 [], replicated
The draws below stay inside these ranges and needn't reach their ends.
Inputs may be any that keep to these rules, and one draw needn't show every extreme that they name: `export_rows`: for each fragment the 4 entries are distinct core rows.
All inputs are finite; a program needn't handle non-finite values.
Results may differ from the reference program's by a relative error of at most 0.0009.
Values may be sent and summed in bfloat16 or wider, within the bound.
No kernel may reach another device: no remote copies, remote signals or barrier semaphores. Data moves between devices by JAX's collectives and lax.ppermute only.
A program may use at most 128 MiB of HBM per device.

```python
import math
import jax
import jax.numpy as jnp
from jax import lax

V = 128
NAUX = 384
P_SIZE = 8
BUF = 2
PASSES = 2
FRAGS = 8


def fragment_rows(key):
    chosen = jax.random.permutation(key, P_SIZE - 2 * BUF)[:2 * BUF]
    return (chosen + BUF).astype(jnp.int32).reshape(2, BUF)


def draw_export_rows(key, part):
    keys = jax.random.split(jax.random.fold_in(key, 17), FRAGS)
    return jax.vmap(fragment_rows)(keys)


def with_ends(drawn, stream_key, smallest, largest):
    dims = drawn.shape
    index_at = [jax.random.randint(jax.random.fold_in(stream_key, axis), (), 0, dims[axis]) for axis in range(len(dims))]
    drawn = drawn.at[tuple(index_at)].set(smallest)
    longest = dims.index(max(dims))
    index_at[longest] = (index_at[longest] + 1) % dims[longest]
    return drawn.at[tuple(index_at)].set(largest)


def level_of(stream_key, dims, cuts, least, high):
    factor_of, own = 1.0, jax.random.fold_in(stream_key, 6)
    for axis_at, blocks in cuts:
        heights = jnp.exp(jax.random.uniform(jax.random.fold_in(own, axis_at), (blocks,), jnp.float32, least / len(cuts), high / len(cuts)))
        factor_of = factor_of * jnp.repeat(heights, dims[axis_at] // blocks).reshape([-1 if axis == axis_at else 1 for axis in range(len(dims))])
    return factor_of


def normal_values(stream_key, extent, deviation, reach, cuts=(), kind=jnp.bfloat16):
    level = level_of(stream_key, extent, cuts, -0.22, 0.18) if cuts else 1.0
    entries = jax.random.normal(stream_key, extent, jnp.float32) * deviation * level
    return jnp.minimum(jnp.maximum(entries, -reach), reach).astype(kind)


def setup_inputs(seed: int = 0) -> dict:
    streams_of = jax.random.split(jax.random.key(seed), 10)
    amps = normal_values(streams_of[0], (FRAGS, V, P_SIZE, V), 0.1, 1.5, ((0, 8), (1, 4)), jnp.float32)
    exch = normal_values(streams_of[1], (FRAGS, V, P_SIZE, V), 0.3, 4.0, ((0, 8), (1, 4)), jnp.float32)
    factors = normal_values(streams_of[2], (FRAGS, NAUX, V, V), (V * NAUX // 16) ** -0.5, 0.109375, ((0, 8), (1, 4)))
    occupied_pair_ladder = normal_values(streams_of[3], (FRAGS, P_SIZE, P_SIZE), (4 * P_SIZE) ** -0.5, 1.0, ((0, 8),), jnp.float32)
    virtual_fock_block = normal_values(streams_of[4], (FRAGS, V, V), (8 * V) ** -0.5, 0.1875, ((0, 8),), jnp.float32)
    virtual_orbital_energy = jnp.clip(1.0 + 2.0 * jax.random.uniform(streams_of[5], (FRAGS, V), jnp.float32) ** level_of(streams_of[5], (FRAGS, V), ((0, 8),), -0.2, 0.2), 1.0, 3.0)
    pair_energy = jnp.clip(-1.5 + 1.0 * jax.random.uniform(streams_of[6], (FRAGS, P_SIZE), jnp.float32) ** level_of(streams_of[6], (FRAGS, P_SIZE), ((0, 8),), -0.2, 0.2), -1.5, -0.5)
    energy_weight = with_ends(jax.random.randint(streams_of[7], (FRAGS, P_SIZE), 0, 3), jax.random.fold_in(streams_of[7], 1), 0, 2).astype(jnp.int32)
    export_rows = draw_export_rows(jax.random.fold_in(streams_of[9], 71), 0)
    return dict(amps=amps, exch=exch, factors=factors, occupied_pair_ladder=occupied_pair_ladder, virtual_fock_block=virtual_fock_block, virtual_orbital_energy=virtual_orbital_energy, pair_energy=pair_energy, energy_weight=energy_weight, export_rows=export_rows)


def ladder_term(factor_whole, cluster_amplitude):
    block_size = math.gcd(NAUX, 48)
    low_amps = lax.optimization_barrier(cluster_amplitude.astype(jnp.bfloat16)).astype(jnp.float32)
    flat_amps = low_amps.reshape(V, P_SIZE * V)
    total = jnp.zeros((V, P_SIZE, V), jnp.float32)
    for block_index in range(NAUX // block_size):
        lower_edge = block_index * block_size
        factor_block = factor_whole[lower_edge:lower_edge + block_size]
        half_done = jnp.dot(factor_block.reshape(block_size * V, V), flat_amps, preferred_element_type=jnp.float32, precision=lax.Precision.HIGHEST)
        half_done = lax.optimization_barrier(half_done.astype(jnp.bfloat16)).astype(jnp.float32)
        half_done = half_done.reshape(block_size, V, P_SIZE, V)
        total = total + jnp.einsum('qapd,qbd->apb', half_done, factor_block, precision=lax.Precision.HIGHEST)
    return total

def one_fragment(inputs):
    amps, exch, factors, occupied_pair_ladder, virtual_fock_block, virtual_orbital_energy, pair_energy = inputs
    factor_whole = factors.astype(jnp.float32)
    denominator = virtual_orbital_energy[:, None, None] + virtual_orbital_energy[None, None, :] - pair_energy[None, :, None]
    cluster_amplitude = amps
    norms = []
    for sweep_index in range(PASSES):
        ladder = ladder_term(factor_whole, cluster_amplitude)
        hole = jnp.einsum('pr,arb->apb', occupied_pair_ladder, cluster_amplitude, precision=lax.Precision.HIGHEST)
        fock_section = jnp.einsum('vn,nog->vog', virtual_fock_block, cluster_amplitude, precision=lax.Precision.HIGHEST)
        fock_section = fock_section + jnp.einsum('apc,bc->apb', cluster_amplitude, virtual_fock_block, precision=lax.Precision.HIGHEST)
        residual = exch + ladder + hole + fock_section - denominator * cluster_amplitude
        norms.append(jnp.sqrt(jnp.sum(residual * residual)))
        cluster_amplitude = cluster_amplitude + residual / denominator
    return (cluster_amplitude, jnp.stack(norms))

def pick_rows(cluster_amplitude, picked):
    return jnp.take(cluster_amplitude, picked, axis=1)

def reference(amps, exch, factors, occupied_pair_ladder, virtual_fock_block, virtual_orbital_energy, pair_energy, energy_weight, export_rows):
    all_amps, res_norms = lax.map(one_fragment, (amps, exch, factors, occupied_pair_ladder, virtual_fock_block, virtual_orbital_energy, pair_energy))
    upward = jax.vmap(pick_rows)(all_amps, export_rows[:, 0, :])
    downward = jax.vmap(pick_rows)(all_amps, export_rows[:, 1, :])
    lower = jnp.concatenate([all_amps[:1, :, :BUF], upward[:-1]], axis=0)
    upper = jnp.concatenate([downward[1:], all_amps[-1:, :, P_SIZE - BUF:]], axis=0)
    new_amps = jnp.concatenate([lower, all_amps[:, :, BUF:P_SIZE - BUF], upper], axis=2)
    weights = energy_weight.astype(jnp.float32) * 0.5
    energy = -jnp.sum(weights[:, None, :, None] * new_amps * exch) / (V * V)
    return (new_amps, res_norms, energy)
```

```python
import functools

import jax
import jax.numpy as jnp
from jax import lax
from jax.experimental import pallas as pl
from jax.experimental.pallas import tpu as pltpu
from jax.sharding import PartitionSpec as P

PASSES = 2
CROSS = 2
F32 = jnp.float32
BF16 = jnp.bfloat16

VMEM = pl.BlockSpec(memory_space=pltpu.VMEM)
SMEM = pl.BlockSpec(memory_space=pltpu.SMEM)
ANY = pl.BlockSpec(memory_space=pl.ANY)


def swap(value, step):
    count = lax.axis_size("blk")
    return lax.ppermute(value, "blk", [(at, at ^ step) for at in range(count)])


def shift(value, axis, steps):
    count = lax.axis_size(axis)
    first, last = max(0, -steps), min(count, count - steps)
    return lax.ppermute(value, axis, [(at, at + steps) for at in range(first, last)])


def call(body, name, out_shape, specs, *args, scratch=(), **params):
    return pl.pallas_call(
        body,
        name=name,
        out_shape=out_shape,
        in_specs=specs,
        out_specs=jax.tree.map(lambda _: VMEM, out_shape),
        scratch_shapes=scratch,
        compiler_params=pltpu.CompilerParams(**params),
    )(*args)


def shaped(*dims, dtype=F32):
    return jax.ShapeDtypeStruct(dims, dtype)


def open_body(meta, occ, amps, exch, fock, eps, keep, send, level, fock_low):
    pairs = amps.shape[1]
    half_count = pairs // 2
    half = meta[2]
    amp = [amps[:, p, :] for p in range(pairs)]
    for p in range(pairs):
        integral = exch[:, p, :]
        local = integral
        for r in range(pairs):
            local = local + occ[p, r] * amp[r]
        at = p % half_count

        @pl.when(half == p // half_count)
        def _():
            keep[0, at], keep[1, at], keep[2, at] = amp[p], integral, local

        @pl.when(half != p // half_count)
        def _():
            send[0, at], send[1, at], send[2, at] = amp[p], integral, local

    wide = jnp.broadcast_to(eps[...], level.shape)
    level[...] = wide + wide.T
    scaled = fock[...] * 0.5
    high = scaled.astype(BF16)
    fock_low[0] = high
    fock_low[1] = (scaled - high.astype(F32)).astype(BF16)


def low_body(meta, keep, came, low):
    rows = keep.shape[2]
    core = meta[0]
    low[:, pl.ds(pl.multiple_of(core * rows, rows), rows), :] = keep[0].astype(BF16)
    low[:, pl.ds(pl.multiple_of((1 - core) * rows, rows), rows), :] = came[0].astype(BF16)


def times_fock(amp, fock):
    half_count, rows, virt = amp.shape
    return lax.dot_general(
        amp.reshape(half_count * rows, virt),
        fock,
        (((1,), (1,)), ((), ())),
        precision=lax.Precision.HIGHEST,
        preferred_element_type=F32,
    ).reshape(half_count, rows, virt)


def start_body(meta, pair, keep, came, fock, level, amp, exch, base, forward):
    half_count, rows = keep.shape[1:3]
    core, chip, half = meta[0], meta[1], meta[2]
    mine = pl.ds(pl.multiple_of(core * rows, rows), rows)
    mate = pl.ds(pl.multiple_of((1 - core) * rows, rows), rows)
    for ref, at in ((amp, 0), (exch, 1), (base, 2)):
        ref[:, mine, :] = keep[at]
        ref[:, mate, :] = came[at]
    turned = times_fock(amp[...], fock[...])
    both = 2 * rows
    levels = level[pl.ds(pl.multiple_of(chip * both, both), both), :]
    for p in range(half_count):
        denominator = levels - pair[half * half_count + p]
        total = base[p] + turned[p] - denominator * amp[p]
        base[p] = total
        forward[p] = amp[p] + total / denominator


def hole_body(meta, occ, pair, amp, other, exch, fock, level, base):
    half_count, rows, _ = amp.shape
    chip, half = meta[1], meta[2]
    turned = times_fock(amp[...], fock[...])
    levels = level[pl.ds(pl.multiple_of(chip * rows, rows), rows), :]
    for p in range(half_count):
        at = half * half_count + p
        total = exch[p] + turned[p] - (levels - pair[at]) * amp[p]
        for r in range(half_count):
            total = total + occ[at, half * half_count + r] * amp[r]
            total = total + occ[at, (1 - half) * half_count + r] * other[r]
        base[p] = total


def ladder_body(meta, fock_low, low_mine, low_other, near, far, *rest, group, closing):
    outs, (slab, turned, half_done, total, sems) = rest[:-5], rest[-5:]
    half_count, rows, virt = low_mine.shape
    aux = near.shape[0]
    steps = aux // group
    chip = meta[1]
    copies = []
    for at in range(2 * steps):
        source = near if at < steps else far
        copies.append(
            pltpu.make_async_copy(
                source.at[pl.ds((at % steps) * group, group)],
                slab.at[pl.ds(at * group, group)],
                sems.at[at],
            )
        )
    for copy in copies:
        copy.start()

    for p in range(half_count):
        first = jnp.where(chip == 0, low_mine[p], low_other[p]).astype(F32)
        second = jnp.where(chip == 0, low_other[p], low_mine[p]).astype(F32)
        whole = jnp.concatenate([first, second], axis=0)
        turned[p * virt : (p + 1) * virt] = whole.T.astype(BF16)

    contract_last = (((1,), (1,)), ((), ()))

    def first_half(at, slot):
        for j in range(group // 2):
            two = slab[pl.ds(at * group + 2 * j, 2)].reshape(2 * virt, virt)
            part = lax.dot_general(
                turned[...], two, contract_last, preferred_element_type=F32
            ).astype(BF16)
            for p in range(half_count):
                for q in range(2):
                    half_done[
                        slot,
                        (2 * j + q) * virt : (2 * j + q + 1) * virt,
                        p * virt : (p + 1) * virt,
                    ] = part[p * virt : (p + 1) * virt, q * virt : (q + 1) * virt]

    def second_half(at, slot):
        across = jnp.concatenate([slab[at * group + q] for q in range(group)], axis=1)
        total[...] += jnp.dot(across, half_done[slot], preferred_element_type=F32)

    fock_part = lax.dot_general(
        turned[...],
        fock_low[...].reshape(2 * virt, virt),
        contract_last,
        preferred_element_type=F32,
    )
    for p in range(half_count):
        block = fock_part[p * virt : (p + 1) * virt]
        total[:, p * virt : (p + 1) * virt] = block[:, :virt] + block[:, virt:]

    copies[0].wait()
    first_half(0, 0)

    def step(at, carry):
        pltpu.make_async_copy(
            near.at[pl.ds(0, group)], slab.at[pl.ds(at * group, group)], sems.at[at]
        ).wait()
        second_half(at - 1, (at - 1) % 2)
        first_half(at, at % 2)
        return carry

    lax.fori_loop(1, 2 * steps, step, 0)
    second_half(2 * steps - 1, (2 * steps - 1) % 2)
    for p in range(half_count):
        block = total[:, p * virt : (p + 1) * virt].T
        if closing:
            send, keep = outs
            top, bottom = block[:rows], block[rows:]
            keep[p] = jnp.where(chip == 0, top, bottom)
            send[p] = jnp.where(chip == 0, bottom, top).astype(BF16)
        else:
            outs[0][p] = block.astype(BF16)


def ladder(meta, fock_low, low_mine, low_other, near, far, closing):
    half_count, rows, virt = low_mine.shape
    aux = near.shape[0]
    group = max(g for g in range(2, 18, 2) if aux % g == 0)
    if closing:
        out = (shaped(half_count, rows, virt, dtype=BF16), shaped(half_count, rows, virt))
    else:
        out = (shaped(half_count, virt, virt, dtype=BF16),)
    return call(
        functools.partial(ladder_body, group=group, closing=closing),
        "ladder",
        out,
        (SMEM, VMEM, VMEM, VMEM, ANY, ANY),
        meta,
        fock_low,
        low_mine,
        low_other,
        near,
        far,
        scratch=(
            pltpu.VMEM((2 * aux, virt, virt), BF16),
            pltpu.VMEM((half_count * virt, virt), BF16),
            pltpu.VMEM((2, group * virt, half_count * virt), BF16),
            pltpu.VMEM((virt, half_count * virt), F32),
            pltpu.SemaphoreType.DMA((2 * aux // group,)),
        ),
        vmem_limit_bytes=24 * 2**20,
    )


def fold_squares(residual):
    rows, virt = residual.shape
    return jnp.sum((residual * residual).reshape(rows // 8, 8, virt), axis=0)


def middle_body(meta, pair, part, came, level, base, near, far, amp, low_mine, low_other, squares):
    half_count, rows, _ = base.shape
    chip, half = meta[1], meta[2]
    mine = pl.ds(pl.multiple_of(chip * rows, rows), rows)
    other = pl.ds(pl.multiple_of((1 - chip) * rows, rows), rows)
    norm = jnp.zeros(squares.shape, F32)
    for p in range(half_count):
        shift_by = pair[half * half_count + p]
        lad = part[p, mine, :].astype(F32) + came[p, mine, :].astype(F32)
        fresh = near[p] + lad / (level[mine, :] - shift_by)
        norm = norm + fold_squares(base[p] + lad)
        amp[p] = fresh
        low_mine[p] = fresh.astype(BF16)
        lad = part[p, other, :].astype(F32) + came[p, other, :].astype(F32)
        low_other[p] = (far[p] + lad / (level[other, :] - shift_by)).astype(BF16)
    squares[...] = norm


def last_body(meta, pair, part, came, level, base, amp, keep, send, squares):
    half_count, rows, _ = base.shape
    core, chip, half = meta[0], meta[1], meta[2]
    single = rows // 2
    levels = level[pl.ds(pl.multiple_of(chip * rows, rows), rows), :]
    norm = jnp.zeros(squares.shape, F32)
    for p in range(half_count):
        residual = base[p] + part[p] + came[p].astype(F32)
        norm = norm + fold_squares(residual)
        fresh = amp[p] + residual / (levels - pair[half * half_count + p])
        top, bottom = fresh[:single], fresh[single:]
        keep[p] = jnp.where(core == 0, top, bottom)
        send[p] = jnp.where(core == 0, bottom, top)
    squares[...] = norm


def border_body(meta, picked, keep, came, whole, upward, downward):
    half_count = keep.shape[0]
    half = meta[2]
    for p in range(half_count):
        whole[half * half_count + p] = keep[p]
        whole[(1 - half) * half_count + p] = came[p]
    for r in range(upward.shape[0]):
        upward[r] = whole[picked[0, r]]
        downward[r] = whole[picked[1, r]]


def close_body(meta, weight, whole, left, right, exch, first, second, new, sums):
    pairs = whole.shape[0]
    border = left.shape[0]
    at_start, at_end = meta[3] == 0, meta[3] == meta[4]
    energy = jnp.zeros(whole.shape[1:], F32)
    for p in range(pairs):
        row = whole[p]
        if p < border:
            row = jnp.where(at_start, row, left[p])
        if p >= pairs - border:
            row = jnp.where(at_end, row, right[p - (pairs - border)])
        new[:, p, :] = row
        energy = energy + (weight[p].astype(F32) * 0.5) * row * exch[:, p, :]
    sums[0:1] = jnp.broadcast_to(jnp.sum(energy), (1, sums.shape[1]))
    sums[1:2] = jnp.broadcast_to(jnp.sum(first[...]), (1, sums.shape[1]))
    sums[2:3] = jnp.broadcast_to(jnp.sum(second[...]), (1, sums.shape[1]))
    sums[3:] = jnp.zeros((sums.shape[0] - 3, sums.shape[1]), F32)


def on_device(
    amps,
    exch,
    factors,
    occupied_pair_ladder,
    virtual_fock_block,
    virtual_orbital_energy,
    pair_energy,
    energy_weight,
    export_rows,
):
    _, row_count, pairs, virt = amps.shape
    half_count = pairs // 2
    both = 2 * row_count
    place = lax.axis_index("blk")
    core, chip = place % 2, place // 2
    half = core ^ chip if CROSS == 3 else core
    frag = lax.axis_index("frag")
    last = jnp.full_like(frag, lax.axis_size("frag") - 1)
    meta = jnp.stack([core, chip, half, frag, last]).astype(jnp.int32)
    occ, fock, pair = occupied_pair_ladder[0], virtual_fock_block[0], pair_energy[0]
    near = factors[0]

    keep, send, level, fock_low = call(
        open_body,
        "open",
        (
            shaped(3, half_count, row_count, virt),
            shaped(3, half_count, row_count, virt),
            shaped(virt, virt),
            shaped(2, virt, virt, dtype=BF16),
        ),
        (SMEM, SMEM, VMEM, VMEM, VMEM, VMEM),
        meta,
        occ,
        amps[0],
        exch[0],
        fock,
        virtual_orbital_energy,
    )
    came = swap(send, 1)
    far = swap(near, 1)
    low_mine = call(
        low_body,
        "low",
        shaped(half_count, both, virt, dtype=BF16),
        (SMEM, VMEM, VMEM),
        meta,
        keep,
        came,
    )
    low_other = swap(low_mine, CROSS)
    own = shaped(half_count, both, virt)
    amp, integral, base, forward = call(
        start_body,
        "start",
        (own, own, own, own),
        (SMEM, SMEM, VMEM, VMEM, VMEM, VMEM),
        meta,
        pair,
        keep,
        came,
        fock,
        level,
    )
    forward_other = swap(forward, CROSS)

    (part,) = ladder(meta, fock_low, low_mine, low_other, near, far, False)
    part_came = swap(part, CROSS)
    small = shaped(8, virt)
    own_low = shaped(half_count, both, virt, dtype=BF16)
    amp, low_mine, low_other, first = call(
        middle_body,
        "middle",
        (own, own_low, own_low, small),
        (SMEM, SMEM, VMEM, VMEM, VMEM, VMEM, VMEM, VMEM),
        meta,
        pair,
        part,
        part_came,
        level,
        base,
        forward,
        forward_other,
    )
    mate_amp = swap(amp, 1)
    send, part = ladder(meta, fock_low, low_mine, low_other, near, far, True)
    part_came = swap(send, CROSS)
    base = call(
        hole_body,
        "hole",
        own,
        (SMEM, SMEM, SMEM, VMEM, VMEM, VMEM, VMEM, VMEM),
        meta,
        occ,
        pair,
        amp,
        mate_amp,
        integral,
        fock,
        level,
    )
    single = shaped(half_count, row_count, virt)
    keep, send, second = call(
        last_body,
        "last",
        (single, single, small),
        (SMEM, SMEM, VMEM, VMEM, VMEM, VMEM, VMEM),
        meta,
        pair,
        part,
        part_came,
        level,
        base,
        amp,
    )
    came = swap(send, 1)
    border = export_rows.shape[2]
    edge = shaped(border, row_count, virt)
    whole, upward, downward = call(
        border_body,
        "border",
        (shaped(pairs, row_count, virt), edge, edge),
        (SMEM, SMEM, VMEM, VMEM),
        meta,
        export_rows[0],
        keep,
        came,
    )
    from_left = shift(upward, "frag", 1)
    from_right = shift(downward, "frag", -1)
    new, sums = call(
        close_body,
        "close",
        (shaped(row_count, pairs, virt), small),
        (SMEM, SMEM, VMEM, VMEM, VMEM, VMEM, VMEM, VMEM),
        meta,
        energy_weight[0],
        whole,
        from_left,
        from_right,
        exch[0],
        first,
        second,
    )
    step = 1
    while step < lax.axis_size("blk"):
        sums = sums + swap(sums, step)
        step *= 2
    norms = jnp.sqrt(sums[1:3, 0])
    energy = sums[0:1]
    step, count = 1, lax.axis_size("frag")
    while step < count:
        energy = energy + lax.ppermute(energy, "frag", [(at, at ^ step) for at in range(count)])
        step *= 2
    energy = -energy[0, 0] / (virt * virt)
    return new[None], norms[None], energy


def solution(mesh):
    placed = (
        P("frag", "blk", None, None),
        P("frag", "blk", None, None),
        P("frag", "blk", None, None),
        P("frag", None, None),
        P("frag", None, None),
        P("frag", None),
        P("frag", None),
        P("frag", None),
        P("frag", None, None),
    )
    return jax.shard_map(
        on_device,
        mesh=mesh,
        in_specs=placed,
        out_specs=(P("frag", "blk", None, None), P("frag", None), P()),
        check_vma=False,
    )
```

```python
import functools

import jax
import jax.numpy as jnp
from jax import lax
from jax.experimental import pallas as pl
from jax.experimental.pallas import tpu as pltpu
from jax.sharding import PartitionSpec as P

PASSES = 2
CROSS = 3
F32 = jnp.float32
BF16 = jnp.bfloat16

VMEM = pl.BlockSpec(memory_space=pltpu.VMEM)
SMEM = pl.BlockSpec(memory_space=pltpu.SMEM)
HBM = pl.BlockSpec(memory_space=pltpu.HBM)


def swap(value, step):
    count = lax.axis_size("blk")
    return lax.ppermute(value, "blk", [(at, at ^ step) for at in range(count)])


def even_swap(value):
    count = lax.axis_size("frag")
    return lax.ppermute(value, "frag", [(at, at ^ 1) for at in range(count)])


def odd_swap(value, closed):
    count = lax.axis_size("frag")
    links = []
    for at in range(count):
        to = at + (1 if at % 2 else -1)
        links.append((at, to % count if closed or 0 <= to < count else at))
    return lax.ppermute(value, "frag", links)


def wide_swap(value, frag_step):
    count = lax.axis_size("blk")
    links = [
        (f * count + b, (f ^ frag_step) * count + (b ^ 1))
        for f in range(lax.axis_size("frag"))
        for b in range(count)
    ]
    return lax.ppermute(value, ("frag", "blk"), links)


def call(body, name, out_shape, specs, *args, scratch=(), limit=6):
    args = [
        pltpu.with_memory_space_constraint(arg, pltpu.HBM) if spec is HBM else arg
        for spec, arg in zip(specs, args, strict=True)
    ]
    return pl.pallas_call(
        body,
        name=name,
        out_shape=out_shape,
        in_specs=specs,
        out_specs=jax.tree.map(lambda _: VMEM, out_shape),
        scratch_shapes=scratch,
        compiler_params=pltpu.CompilerParams(vmem_limit_bytes=limit * 2**20),
    )(*args)


def shaped(*dims, dtype=F32):
    return jax.ShapeDtypeStruct(dims, dtype)


def times_fock(amp, fock):
    return lax.dot_general(
        amp,
        fock,
        (((1,), (1,)), ((), ())),
        precision=lax.Precision.HIGHEST,
        preferred_element_type=F32,
    )


def join(keep_first, keep, came):
    return jnp.where(
        keep_first,
        jnp.concatenate([keep, came], axis=0),
        jnp.concatenate([came, keep], axis=0),
    )


def open_body(
    meta,
    occ_in,
    weight_in,
    pair_in,
    amps_in,
    exch_in,
    fock_in,
    eps_in,
    low_keep,
    low_send,
    keep,
    send,
    level,
    fock_low,
    own,
    even_weights,
    odd_weights,
    occ,
    weight,
    pair,
    amps,
    exch,
    fock,
    eps,
    sems,
):
    moves = (
        (amps_in, amps),
        (exch_in, exch),
        (occ_in, occ),
        (weight_in, weight),
        (pair_in, pair),
        (fock_in, fock),
        (eps_in, eps),
    )
    copies = [pltpu.make_async_copy(*move, sems.at[at]) for at, move in enumerate(moves)]
    for copy in copies:
        copy.start()
    for copy in copies:
        copy.wait()
    rows, pairs, virt = amps.shape
    half_count = pairs // 2
    border = even_weights.shape[0]
    half = meta[2]
    at_start, at_end = meta[3] == 0, meta[3] == meta[4]
    is_even = meta[3] % 2 == 0
    wide = jnp.broadcast_to(eps[...], level.shape)
    level[...] = wide + wide.T
    levels = level[pl.ds(pl.multiple_of(meta[5] * rows, rows), rows), :]
    amp = [amps[:, p, :] for p in range(pairs)]
    turned = times_fock(jnp.concatenate(amp, axis=0), fock[...])
    for p in range(pairs):
        integral = exch[:, p, :]
        denominator = levels - pair[0, p]
        base = integral + turned[p * rows : (p + 1) * rows] - denominator * amp[p]
        for r in range(pairs):
            base = base + occ[p, r] * amp[r]
        forward = amp[p] + base / denominator
        low = amp[p].astype(BF16)
        at = p % half_count

        @pl.when(half == p // half_count)
        def _():
            low_keep[at] = low
            keep[0, at], keep[1, at], keep[2, at] = integral, base, forward

        @pl.when(half != p // half_count)
        def _():
            low_send[at] = low
            send[0, at], send[1, at], send[2, at] = integral, base, forward

        weighted = (weight[0, p].astype(F32) * 0.5) * integral
        if p < border:

            @pl.when(is_even)
            def _():
                odd_weights[p] = weighted

            @pl.when(jnp.logical_not(is_even))
            def _():
                even_weights[p] = weighted

            weighted = jnp.where(at_start, weighted, 0.0)
        if p >= pairs - border:

            @pl.when(is_even)
            def _():
                even_weights[p - (pairs - border)] = weighted

            @pl.when(jnp.logical_not(is_even))
            def _():
                odd_weights[p - (pairs - border)] = weighted

            weighted = jnp.where(at_end, weighted, 0.0)
        own[p] = weighted

    scaled = fock[...] * 0.5
    high = scaled.astype(BF16)
    fock_low[0] = high
    fock_low[1] = (scaled - high.astype(F32)).astype(BF16)


def hole_body(meta, occ, pair, amp, from_mate, keep, came, fock, level, base):
    half_count, rows, virt = amp.shape
    core, chip, half = meta[0], meta[1], meta[2]
    turned = times_fock(amp[...].reshape(half_count * rows, virt), fock[...])
    levels = level[pl.ds(pl.multiple_of(chip * rows, rows), rows), :]
    for p in range(half_count):
        at = half * half_count + p
        total = join(core == 0, keep[0, p], came[0, p])
        total = total + turned[p * rows : (p + 1) * rows] - (levels - pair[at]) * amp[p]
        for r in range(half_count):
            total = total + occ[at, half * half_count + r] * amp[r]
            total = total + occ[at, (1 - half) * half_count + r] * from_mate[r, :rows, :]
        base[p] = total


def ladder_body(meta, fock_low, *rest, group, closing, count):
    lows, (source, far), rest = rest[:count], rest[count : count + 2], rest[count + 2 :]
    outs, (near, gathered, turned, half_done, total, sem) = rest[:-6], rest[-6:]
    fetch = pltpu.make_async_copy(source, near, sem)
    fetch.start()
    half_count, rows, virt = lows[0].shape
    steps = far.shape[0] // group
    chip = meta[1]
    if count == 1:
        gathered = lows[0]
    else:
        for low, offset in zip(lows, (0, 1, CROSS, CROSS ^ 1), strict=True):
            at = jnp.bitwise_xor(meta[5], offset)
            gathered[:, pl.ds(pl.multiple_of(at * rows, rows), rows), :] = low[...]
    rows = virt // 2
    for p in range(half_count):
        turned[p * virt : (p + 1) * virt] = gathered[p].astype(F32).T.astype(BF16)

    contract_last = (((1,), (1,)), ((), ()))

    def first_half(slab, at, slot):
        for j in range(group // 2):
            two = slab[pl.ds(at * group + 2 * j, 2)].reshape(2 * virt, virt)
            part = lax.dot_general(
                turned[...], two, contract_last, preferred_element_type=F32
            ).astype(BF16)
            for p in range(half_count):
                for q in range(2):
                    half_done[
                        slot,
                        (2 * j + q) * virt : (2 * j + q + 1) * virt,
                        p * virt : (p + 1) * virt,
                    ] = part[p * virt : (p + 1) * virt, q * virt : (q + 1) * virt]

    def second_half(slab, at, slot):
        across = jnp.concatenate([slab[at * group + q] for q in range(group)], axis=1)
        total[...] += jnp.dot(across, half_done[slot], preferred_element_type=F32)

    fock_part = lax.dot_general(
        turned[...],
        fock_low[...].reshape(2 * virt, virt),
        contract_last,
        preferred_element_type=F32,
    )
    for p in range(half_count):
        block = fock_part[p * virt : (p + 1) * virt]
        total[:, p * virt : (p + 1) * virt] = block[:, :virt] + block[:, virt:]

    def sweep(slab, offset):
        def step(at, carry):
            second_half(slab, at - 1, (offset + at - 1) % 2)
            first_half(slab, at, (offset + at) % 2)
            return carry

        lax.fori_loop(1, steps, step, 0)

    first_half(far, 0, 0)
    sweep(far, 0)
    fetch.wait()
    second_half(far, steps - 1, (steps - 1) % 2)
    first_half(near, 0, steps % 2)
    sweep(near, steps)
    second_half(near, steps - 1, (2 * steps - 1) % 2)
    for p in range(half_count):
        block = total[:, p * virt : (p + 1) * virt].T
        if closing:
            send, keep = outs
            top, bottom = block[:rows], block[rows:]
            keep[p] = jnp.where(chip == 0, top, bottom)
            send[p] = jnp.where(chip == 0, bottom, top).astype(BF16)
        else:
            outs[0][p] = block.astype(BF16)


def ladder(meta, fock_low, lows, near, far, closing):
    half_count, _, virt = lows[0].shape
    rows = virt // 2
    aux = near.shape[0]
    group = max(g for g in range(2, 50, 2) if aux % g == 0)
    if closing:
        out = (shaped(half_count, rows, virt, dtype=BF16), shaped(half_count, rows, virt))
    else:
        out = (shaped(half_count, virt, virt, dtype=BF16),)
    return call(
        functools.partial(ladder_body, group=group, closing=closing, count=len(lows)),
        "ladder",
        out,
        (SMEM,) + (VMEM,) * (1 + len(lows)) + (HBM, VMEM),
        meta,
        fock_low,
        *lows,
        near,
        far,
        scratch=(
            pltpu.VMEM((aux, virt, virt), BF16),
            pltpu.VMEM((half_count, virt, virt), BF16),
            pltpu.VMEM((half_count * virt, virt), BF16),
            pltpu.VMEM((2, group * virt, half_count * virt), BF16),
            pltpu.VMEM((virt, half_count * virt), F32),
            pltpu.SemaphoreType.DMA(()),
        ),
        limit=28,
    )


def fold_squares(residual):
    rows, virt = residual.shape
    return jnp.sum((residual * residual).reshape(rows // 8, 8, virt), axis=0)


def middle_body(
    meta,
    pair,
    picked,
    part,
    part_came,
    level,
    keep,
    came,
    far,
    own,
    even_came,
    odd_came,
    amp,
    low,
    squares,
    to_mate,
    keep_weights,
    weights,
):
    half_count, rows, _ = amp.shape
    core, chip, half = meta[0], meta[1], meta[2]
    mine = pl.ds(pl.multiple_of(chip * rows, rows), rows)
    other = pl.ds(pl.multiple_of((1 - chip) * rows, rows), rows)
    norm = jnp.zeros(squares.shape, F32)
    far_first = core == (0 if CROSS == 2 else 1)
    for p in range(half_count):
        shift_by = pair[half * half_count + p]
        lad = part[p, mine, :].astype(F32) + part_came[p, mine, :].astype(F32)
        fresh = join(core == 0, keep[2, p], came[2, p]) + lad / (level[mine, :] - shift_by)
        norm = norm + fold_squares(join(core == 0, keep[1, p], came[1, p]) + lad)
        amp[p] = fresh
        to_mate[p, :rows, :] = fresh
        low[p, mine, :] = fresh.astype(BF16)
        lad = part[p, other, :].astype(F32) + part_came[p, other, :].astype(F32)
        fresh = join(far_first, far[0, p], far[1, p]) + lad / (level[other, :] - shift_by)
        low[p, other, :] = fresh.astype(BF16)
    squares[...] = norm
    is_even, at_start, at_end = meta[3] % 2 == 0, meta[3] == 0, meta[3] == meta[4]
    weights[...] = own[...]
    for r in range(even_came.shape[0]):
        above = jnp.where(is_even, even_came[r], odd_came[r])
        below = jnp.where(is_even, odd_came[r], even_came[r])
        at = picked[0, r]
        weights[at] = weights[at] + jnp.where(at_end, 0.0, above)
        at = picked[1, r]
        weights[at] = weights[at] + jnp.where(at_start, 0.0, below)
    for p in range(half_count):
        keep_weights[p] = weights[half * half_count + p]
        to_mate[p, rows:, :] = weights[(1 - half) * half_count + p]


def last_body(
    meta, pair, part, came, level, base, amp, keep_weights, from_mate, first, keep, send
):
    half_count, rows, virt = base.shape
    core, chip, half = meta[0], meta[1], meta[2]
    single = rows // 2
    levels = level[pl.ds(pl.multiple_of(chip * rows, rows), rows), :]
    norm = jnp.zeros(first.shape, F32)
    energy = jnp.zeros((single, virt), F32)
    for p in range(half_count):
        residual = base[p] + part[p] + came[p].astype(F32)
        norm = norm + fold_squares(residual)
        fresh = amp[p] + residual / (levels - pair[half * half_count + p])
        top, bottom = fresh[:single], fresh[single:]
        mine = jnp.where(core == 0, top, bottom)
        mate = jnp.where(core == 0, bottom, top)
        energy = energy + keep_weights[p] * mine + from_mate[p, rows:, :] * mate
        keep[p * single : (p + 1) * single, :] = mine
        send[p * single : (p + 1) * single, :] = mate
    tail = send.shape[0] - half_count * single
    slot = lax.broadcasted_iota(jnp.int32, (tail, virt), 0)
    sums = jnp.where(slot == 0, jnp.sum(energy), 0.0)
    sums = jnp.where(slot == 1, jnp.sum(first[...]), sums)
    sums = jnp.where(slot == 2, jnp.sum(norm), sums)
    keep[half_count * single :, :] = sums
    send[half_count * single :, :] = sums


def border_body(meta, picked, keep, came, whole, even_rows, odd_rows, sums):
    pairs, single, _ = whole.shape
    half_count = pairs // 2
    border = picked.shape[1]
    half = meta[2]
    for p in range(half_count):
        whole[half * half_count + p] = keep[p * single : (p + 1) * single, :]
        whole[(1 - half) * half_count + p] = came[p * single : (p + 1) * single, :]
    parity = meta[3] % 2
    for r in range(border):
        even_rows[r * single : (r + 1) * single, :] = whole[picked[parity, r]]
        odd_rows[r * single : (r + 1) * single, :] = whole[picked[1 - parity, r]]
    sums[...] = keep[half_count * single :, :] + came[half_count * single :, :]


def close_body(meta, whole, even_came, odd_came, new):
    pairs, single, _ = whole.shape
    border = (even_came.shape[0] - 8) // single
    is_even, at_start, at_end = meta[3] % 2 == 0, meta[3] == 0, meta[3] == meta[4]
    for p in range(pairs):
        row = whole[p]
        if p < border:
            block = slice(p * single, (p + 1) * single)
            left = jnp.where(is_even, odd_came[block, :], even_came[block, :])
            row = jnp.where(at_start, row, left)
        if p >= pairs - border:
            at = p - (pairs - border)
            block = slice(at * single, (at + 1) * single)
            right = jnp.where(is_even, even_came[block, :], odd_came[block, :])
            row = jnp.where(at_end, row, right)
        new[:, p, :] = row


def on_device(
    amps,
    exch,
    factors,
    occupied_pair_ladder,
    virtual_fock_block,
    virtual_orbital_energy,
    pair_energy,
    energy_weight,
    export_rows,
):
    _, row_count, pairs, virt = amps.shape
    half_count = pairs // 2
    both = 2 * row_count
    place = lax.axis_index("blk")
    core, chip = place % 2, place // 2
    half = core ^ chip if CROSS == 3 else core
    frag = lax.axis_index("frag")
    last = jnp.full_like(frag, lax.axis_size("frag") - 1)
    meta = jnp.stack([core, chip, half, frag, last, place]).astype(jnp.int32)
    occ, fock, pair = occupied_pair_ladder[0], virtual_fock_block[0], pair_energy[0]
    near = factors[0]

    border = export_rows.shape[2]
    edge = shaped(border, row_count, virt)
    single = shaped(half_count, row_count, virt)
    single_low = shaped(half_count, row_count, virt, dtype=BF16)
    triple = shaped(3, half_count, row_count, virt)
    low_keep, low_send, keep, send, level, fock_low, own_weights, even_weights, odd_weights = call(
        open_body,
        "open",
        (
            single_low,
            single_low,
            triple,
            triple,
            shaped(virt, virt),
            shaped(2, virt, virt, dtype=BF16),
            shaped(pairs, row_count, virt),
            edge,
            edge,
        ),
        (SMEM,) + (HBM,) * 7,
        meta,
        occ,
        energy_weight,
        pair_energy,
        amps[0],
        exch[0],
        fock,
        virtual_orbital_energy,
        scratch=(
            pltpu.SMEM(occ.shape, F32),
            pltpu.SMEM(energy_weight.shape, jnp.int32),
            pltpu.SMEM(pair_energy.shape, F32),
            pltpu.VMEM(amps.shape[1:], F32),
            pltpu.VMEM(amps.shape[1:], F32),
            pltpu.VMEM(fock.shape, F32),
            pltpu.VMEM(virtual_orbital_energy.shape, F32),
            pltpu.SemaphoreType.DMA((7,)),
        ),
    )
    lows = (
        low_keep,
        swap(low_send, 1),
        swap(low_keep, CROSS),
        swap(low_send, CROSS ^ 1),
    )
    far = swap(near, 1)
    came = swap(send, 1)
    forward_other = swap(jnp.stack([keep[2], came[2]]), CROSS)
    own = shaped(half_count, both, virt)
    (part,) = ladder(meta, fock_low, lows, near, far, False)
    part, even_weights, odd_weights = lax.optimization_barrier((part, even_weights, odd_weights))
    part_came = swap(part, CROSS)
    even_came = even_swap(even_weights)
    odd_came = odd_swap(odd_weights, False)
    small = shaped(8, virt)
    low = shaped(half_count, virt, virt, dtype=BF16)
    amp, low, first, to_mate, keep_weights = call(
        middle_body,
        "middle",
        (own, low, small, shaped(half_count, both + row_count, virt), single),
        (SMEM, SMEM, SMEM) + (VMEM,) * 9,
        meta,
        pair,
        export_rows[0],
        part,
        part_came,
        level,
        keep,
        came,
        forward_other,
        own_weights,
        even_came,
        odd_came,
        scratch=(pltpu.VMEM((pairs, row_count, virt), F32),),
    )
    from_mate = swap(to_mate, 1)
    send, part = ladder(meta, fock_low, (low,), near, far, True)
    part_came = swap(send, CROSS)
    base = call(
        hole_body,
        "hole",
        own,
        (SMEM, SMEM, SMEM) + (VMEM,) * 6,
        meta,
        occ,
        pair,
        amp,
        from_mate,
        keep,
        came,
        fock,
        level,
    )
    packed = shaped(half_count * row_count + 8, virt)
    last_keep, send = call(
        last_body,
        "last",
        (packed, packed),
        (SMEM, SMEM) + (VMEM,) * 8,
        meta,
        pair,
        part,
        part_came,
        level,
        base,
        amp,
        keep_weights,
        from_mate,
        first,
    )
    last_came = swap(send, 1)
    rows = shaped(border * row_count, virt)
    whole, even_rows, odd_rows, sums = call(
        border_body,
        "border",
        (shaped(pairs, row_count, virt), rows, rows, small),
        (SMEM, SMEM, VMEM, VMEM),
        meta,
        export_rows[0],
        last_keep,
        last_came,
    )
    sums = sums + swap(sums, CROSS)
    norms = jnp.sqrt(sums[1:3, 0])
    even_came = even_swap(jnp.concatenate([even_rows, sums], axis=0))
    sums = sums + even_came[border * row_count :]
    odd_came = odd_swap(jnp.concatenate([odd_rows, sums], axis=0), True)
    sums = sums + odd_came[border * row_count :]
    step = 4
    while step < lax.axis_size("frag"):
        sums = sums + wide_swap(sums, step)
        step *= 2
    new = call(
        close_body,
        "close",
        shaped(row_count, pairs, virt),
        (SMEM, VMEM, VMEM, VMEM),
        meta,
        whole,
        even_came,
        odd_came,
    )
    energy = -sums[0, 0] / (virt * virt)
    return new[None], norms[None], energy


def solution(mesh):
    placed = (
        P("frag", "blk", None, None),
        P("frag", "blk", None, None),
        P("frag", "blk", None, None),
        P("frag", None, None),
        P("frag", None, None),
        P("frag", None),
        P("frag", None),
        P("frag", None),
        P("frag", None, None),
    )
    return jax.shard_map(
        on_device,
        mesh=mesh,
        in_specs=placed,
        out_specs=(P("frag", "blk", None, None), P("frag", None), P()),
        check_vma=False,
    )
```

```python
import functools

import jax
import jax.numpy as jnp
from jax import lax
from jax.experimental import pallas as pl
from jax.experimental.pallas import tpu as pltpu
from jax.sharding import PartitionSpec as P

PASSES = 2
CROSS = 3
F32 = jnp.float32
BF16 = jnp.bfloat16

VMEM = pl.BlockSpec(memory_space=pltpu.VMEM)
SMEM = pl.BlockSpec(memory_space=pltpu.SMEM)
HBM = pl.BlockSpec(memory_space=pltpu.HBM)


def swap(value, step):
    count = lax.axis_size("blk")
    return lax.ppermute(value, "blk", [(at, at ^ step) for at in range(count)])


def even_swap(value):
    count = lax.axis_size("frag")
    return lax.ppermute(value, "frag", [(at, at ^ 1) for at in range(count)])


def odd_swap(value, closed):
    count = lax.axis_size("frag")
    links = []
    for at in range(count):
        to = at + (1 if at % 2 else -1)
        links.append((at, to % count if closed or 0 <= to < count else at))
    return lax.ppermute(value, "frag", links)


def wide_swap(value, frag_step):
    count = lax.axis_size("blk")
    links = [
        (f * count + b, (f ^ frag_step) * count + (b ^ 1))
        for f in range(lax.axis_size("frag"))
        for b in range(count)
    ]
    return lax.ppermute(value, ("frag", "blk"), links)


def call(body, out_shape, specs, *args, scratch=(), limit=6, flops=0):
    args = [
        pltpu.with_memory_space_constraint(arg, pltpu.HBM) if spec is HBM else arg
        for spec, arg in zip(specs, args, strict=True)
    ]
    return pl.pallas_call(
        body,
        out_shape=out_shape,
        in_specs=specs,
        out_specs=jax.tree.map(lambda _: VMEM, out_shape),
        scratch_shapes=scratch,
        cost_estimate=pl.CostEstimate(flops=flops, bytes_accessed=0, transcendentals=0),
        compiler_params=pltpu.CompilerParams(vmem_limit_bytes=limit * 2**20),
    )(*args)


def shaped(*dims, dtype=F32):
    return jax.ShapeDtypeStruct(dims, dtype)


def times_fock(amp, fock):
    return lax.dot_general(
        amp,
        fock,
        (((1,), (1,)), ((), ())),
        precision=lax.Precision.HIGHEST,
        preferred_element_type=F32,
    )


def join(keep_first, keep, came):
    return jnp.where(
        keep_first,
        jnp.concatenate([keep, came], axis=0),
        jnp.concatenate([came, keep], axis=0),
    )


def early_body(
    meta,
    amps_in,
    exch_in,
    fock_in,
    eps_in,
    occ_in,
    pair_in,
    weight_in,
    low_keep,
    low_send,
    amps,
    exch,
    fock,
    eps,
    occ,
    pair,
    weight,
    sems,
):
    moves = (
        (amps_in, amps),
        (exch_in, exch),
        (fock_in, fock),
        (eps_in, eps),
        (occ_in, occ),
        (pair_in, pair),
        (weight_in, weight),
    )
    copies = [pltpu.make_async_copy(*move, sems.at[at]) for at, move in enumerate(moves)]
    for copy in copies:
        copy.start()
    copies[0].wait()
    half_count = amps.shape[1] // 2
    half = meta[2]
    for p in range(half_count):
        first = amps[:, p, :].astype(BF16)
        second = amps[:, half_count + p, :].astype(BF16)
        low_keep[p] = jnp.where(half == 0, first, second)
        low_send[p] = jnp.where(half == 0, second, first)
    for copy in copies[1:]:
        copy.wait()


def open_body(
    meta,
    occ,
    pair,
    weight,
    amps,
    exch,
    fock,
    eps,
    keep,
    send,
    level,
    fock_low,
    own,
    even_weights,
    odd_weights,
):
    rows, pairs, _ = amps.shape
    half_count = pairs // 2
    border = even_weights.shape[0]
    half = meta[2]
    at_start, at_end = meta[3] == 0, meta[3] == meta[4]
    is_even = meta[3] % 2 == 0
    wide = jnp.broadcast_to(eps[...], level.shape)
    level[...] = wide + wide.T
    levels = level[pl.ds(pl.multiple_of(meta[5] * rows, rows), rows), :]
    amp = [amps[:, p, :] for p in range(pairs)]
    turned = times_fock(jnp.concatenate(amp, axis=0), fock[...])
    for p in range(pairs):
        integral = exch[:, p, :]
        partial = integral + turned[p * rows : (p + 1) * rows]
        for r in range(pairs):
            partial = partial + occ[p, r] * amp[r]
        base = partial - (levels - pair[0, p]) * amp[p]
        at = p % half_count

        @pl.when(half == p // half_count)
        def _():
            keep[0, at], keep[1, at], keep[2, at] = integral, base, partial

        @pl.when(half != p // half_count)
        def _():
            send[0, at], send[1, at], send[2, at] = integral, base, partial

        weighted = (weight[0, p].astype(F32) * 0.5) * integral
        if p < border:

            @pl.when(is_even)
            def _():
                odd_weights[p] = weighted

            @pl.when(jnp.logical_not(is_even))
            def _():
                even_weights[p] = weighted

            weighted = jnp.where(at_start, weighted, 0.0)
        if p >= pairs - border:

            @pl.when(is_even)
            def _():
                even_weights[p - (pairs - border)] = weighted

            @pl.when(jnp.logical_not(is_even))
            def _():
                odd_weights[p - (pairs - border)] = weighted

            weighted = jnp.where(at_end, weighted, 0.0)
        own[p] = weighted

    scaled = fock[...] * 0.5
    high = scaled.astype(BF16)
    fock_low[0] = high
    fock_low[1] = (scaled - high.astype(F32)).astype(BF16)


def hole_body(meta, occ, pair, amp, from_mate, keep, came, fock, level, base):
    half_count, rows, virt = amp.shape
    core, chip, half = meta[0], meta[1], meta[2]
    turned = times_fock(amp[...].reshape(half_count * rows, virt), fock[...])
    levels = level[pl.ds(pl.multiple_of(chip * rows, rows), rows), :]
    for p in range(half_count):
        at = half * half_count + p
        total = join(core == 0, keep[0, p], came[0, p])
        total = total + turned[p * rows : (p + 1) * rows] - (levels - pair[0, at]) * amp[p]
        for r in range(half_count):
            total = total + occ[at, half * half_count + r] * amp[r]
            total = total + occ[at, (1 - half) * half_count + r] * from_mate[r, :rows, :]
        base[p] = total


def ladder_body(meta, fock_low, *rest, group, count):
    lows, (source, far), rest = rest[:count], rest[count : count + 2], rest[count + 2 :]
    closing = count == 1
    if not closing:
        (keep, came), rest = rest[:2], rest[2:]
    outs, (near, gathered, turned, half_done, total, sem) = rest[:-6], rest[-6:]
    fetch = pltpu.make_async_copy(source, near, sem)
    fetch.start()
    half_count, rows, virt = lows[0].shape
    steps = far.shape[0] // group
    chip = meta[1]
    if count == 1:
        gathered = lows[0]
    else:
        for low, offset in zip(lows, (0, 1, CROSS, CROSS ^ 1), strict=True):
            at = jnp.bitwise_xor(meta[5], offset)
            gathered[:, pl.ds(pl.multiple_of(at * rows, rows), rows), :] = low[...]
    rows = virt // 2
    for p in range(half_count):
        turned[p * virt : (p + 1) * virt] = gathered[p].astype(F32).T.astype(BF16)

    contract_last = (((1,), (1,)), ((), ()))

    def first_half(slab, at, slot):
        for j in range(group // 2):
            two = slab[pl.ds(at * group + 2 * j, 2)].reshape(2 * virt, virt)
            part = lax.dot_general(
                turned[...], two, contract_last, preferred_element_type=F32
            ).astype(BF16)
            for p in range(half_count):
                for q in range(2):
                    half_done[
                        slot,
                        (2 * j + q) * virt : (2 * j + q + 1) * virt,
                        p * virt : (p + 1) * virt,
                    ] = part[p * virt : (p + 1) * virt, q * virt : (q + 1) * virt]

    def second_half(slab, at, slot):
        across = jnp.concatenate([slab[at * group + q] for q in range(group)], axis=1)
        total[...] += jnp.dot(across, half_done[slot], preferred_element_type=F32)

    fock_part = lax.dot_general(
        turned[...],
        fock_low[...].reshape(2 * virt, virt),
        contract_last,
        preferred_element_type=F32,
    )
    for p in range(half_count):
        block = fock_part[p * virt : (p + 1) * virt]
        total[:, p * virt : (p + 1) * virt] = block[:, :virt] + block[:, virt:]

    def sweep(slab, offset):
        def step(at, carry):
            second_half(slab, at - 1, (offset + at - 1) % 2)
            first_half(slab, at, (offset + at) % 2)
            return carry

        lax.fori_loop(1, steps, step, 0)

    first_half(far, 0, 0)
    sweep(far, 0)
    fetch.wait()
    second_half(far, steps - 1, (steps - 1) % 2)
    first_half(near, 0, steps % 2)
    sweep(near, steps)
    second_half(near, steps - 1, (2 * steps - 1) % 2)
    for p in range(half_count):
        block = total[:, p * virt : (p + 1) * virt].T
        top, bottom = block[:rows], block[rows:]
        if closing:
            send, kept = outs
            kept[p] = jnp.where(chip == 0, top, bottom)
            send[p] = jnp.where(chip == 0, bottom, top).astype(BF16)
        else:
            part, send = outs
            part[p] = block
            extra = join(meta[0] == 0, keep[2, p], came[2, p])
            send[p, :rows, :] = (top + jnp.where(chip == 0, extra, 0.0)).astype(BF16)
            send[p, rows:, :] = (bottom + jnp.where(chip == 0, 0.0, extra)).astype(BF16)


def ladder(meta, fock_low, lows, near, far, *own):
    half_count, _, virt = lows[0].shape
    rows = virt // 2
    aux = near.shape[0]
    group = max(g for g in range(2, 50, 2) if aux % g == 0)
    if own:
        out = (shaped(half_count, virt, virt), shaped(half_count, virt, virt, dtype=BF16))
    else:
        out = (shaped(half_count, rows, virt, dtype=BF16), shaped(half_count, rows, virt))
    return call(
        functools.partial(ladder_body, group=group, count=len(lows)),
        out,
        (SMEM,) + (VMEM,) * (1 + len(lows)) + (HBM, VMEM) + (VMEM,) * len(own),
        meta,
        fock_low,
        *lows,
        near,
        far,
        *own,
        scratch=(
            pltpu.VMEM((aux, virt, virt), BF16),
            pltpu.VMEM((half_count, virt, virt), BF16),
            pltpu.VMEM((half_count * virt, virt), BF16),
            pltpu.VMEM((2, group * virt, half_count * virt), BF16),
            pltpu.VMEM((virt, half_count * virt), F32),
            pltpu.SemaphoreType.DMA(()),
        ),
        limit=28,
        flops=8 * aux * half_count * virt**3,
    )


def fold_squares(residual):
    rows, virt = residual.shape
    return jnp.sum((residual * residual).reshape(rows // 8, 8, virt), axis=0)


def middle_body(
    meta,
    pair,
    picked,
    part,
    part_came,
    level,
    keep,
    came,
    own,
    even_came,
    odd_came,
    amp,
    low,
    squares,
    to_mate,
    keep_weights,
    weights,
):
    half_count, rows, _ = amp.shape
    core, chip, half = meta[0], meta[1], meta[2]
    mine = pl.ds(pl.multiple_of(chip * rows, rows), rows)
    other = pl.ds(pl.multiple_of((1 - chip) * rows, rows), rows)
    norm = jnp.zeros(squares.shape, F32)
    for p in range(half_count):
        shift_by = pair[0, half * half_count + p]
        lad = part[p, mine, :] + part_came[p, mine, :].astype(F32)
        fresh = (join(core == 0, keep[2, p], came[2, p]) + lad) / (level[mine, :] - shift_by)
        norm = norm + fold_squares(join(core == 0, keep[1, p], came[1, p]) + lad)
        amp[p] = fresh
        to_mate[p, :rows, :] = fresh
        low[p, mine, :] = fresh.astype(BF16)
        total = part[p, other, :] + part_came[p, other, :].astype(F32)
        low[p, other, :] = (total / (level[other, :] - shift_by)).astype(BF16)
    squares[...] = norm
    is_even, at_start, at_end = meta[3] % 2 == 0, meta[3] == 0, meta[3] == meta[4]
    weights[...] = own[...]
    for r in range(even_came.shape[0]):
        above = jnp.where(is_even, even_came[r], odd_came[r])
        below = jnp.where(is_even, odd_came[r], even_came[r])
        at = picked[0, r]
        weights[at] = weights[at] + jnp.where(at_end, 0.0, above)
        at = picked[1, r]
        weights[at] = weights[at] + jnp.where(at_start, 0.0, below)
    for p in range(half_count):
        keep_weights[p] = weights[half * half_count + p]
        to_mate[p, rows:, :] = weights[(1 - half) * half_count + p]


def last_body(
    meta, pair, part, came, level, base, amp, keep_weights, from_mate, first, keep, send, sums_out
):
    half_count, rows, virt = base.shape
    core, chip, half = meta[0], meta[1], meta[2]
    single = rows // 2
    levels = level[pl.ds(pl.multiple_of(chip * rows, rows), rows), :]
    norm = jnp.zeros(first.shape, F32)
    energy = jnp.zeros((single, virt), F32)
    for p in range(half_count):
        residual = base[p] + part[p] + came[p].astype(F32)
        norm = norm + fold_squares(residual)
        fresh = amp[p] + residual / (levels - pair[0, half * half_count + p])
        top, bottom = fresh[:single], fresh[single:]
        mine = jnp.where(core == 0, top, bottom)
        mate = jnp.where(core == 0, bottom, top)
        energy = energy + keep_weights[p] * mine + from_mate[p, rows:, :] * mate
        keep[p * single : (p + 1) * single, :] = mine
        send[p * single : (p + 1) * single, :] = mate
    tail = send.shape[0] - half_count * single
    slot = lax.broadcasted_iota(jnp.int32, (tail, virt), 0)
    sums = jnp.where(slot == 0, jnp.sum(energy), 0.0)
    sums = jnp.where(slot == 1, jnp.sum(first[...]), sums)
    sums = jnp.where(slot == 2, jnp.sum(norm), sums)
    keep[half_count * single :, :] = sums
    send[half_count * single :, :] = sums
    sums_out[...] = sums


def border_body(meta, picked, keep, came, whole, even_rows, odd_rows, sums):
    pairs, single, _ = whole.shape
    half_count = pairs // 2
    border = picked.shape[1]
    half = meta[2]
    for p in range(half_count):
        whole[half * half_count + p] = keep[p * single : (p + 1) * single, :]
        whole[(1 - half) * half_count + p] = came[p * single : (p + 1) * single, :]
    parity = meta[3] % 2
    for r in range(border):
        even_rows[r * single : (r + 1) * single, :] = whole[picked[parity, r]]
        odd_rows[r * single : (r + 1) * single, :] = whole[picked[1 - parity, r]]
    sums[...] = keep[half_count * single :, :] + came[half_count * single :, :]


def close_body(meta, whole, even_came, odd_came, squares, new, norms):
    norms[...] = jnp.sqrt(jnp.concatenate([squares[1:2, 0:1], squares[2:3, 0:1]], axis=1))
    pairs, single, _ = whole.shape
    border = (even_came.shape[0] - 8) // single
    is_even, at_start, at_end = meta[3] % 2 == 0, meta[3] == 0, meta[3] == meta[4]
    for p in range(pairs):
        row = whole[p]
        if p < border:
            block = slice(p * single, (p + 1) * single)
            left = jnp.where(is_even, odd_came[block, :], even_came[block, :])
            row = jnp.where(at_start, row, left)
        if p >= pairs - border:
            at = p - (pairs - border)
            block = slice(at * single, (at + 1) * single)
            right = jnp.where(is_even, even_came[block, :], odd_came[block, :])
            row = jnp.where(at_end, row, right)
        new[:, p, :] = row


def on_device(
    amps,
    exch,
    factors,
    occupied_pair_ladder,
    virtual_fock_block,
    virtual_orbital_energy,
    pair_energy,
    energy_weight,
    export_rows,
):
    _, row_count, pairs, virt = amps.shape
    half_count = pairs // 2
    both = 2 * row_count
    place = lax.axis_index("blk")
    core, chip = place % 2, place // 2
    half = core ^ chip if CROSS == 3 else core
    frag = lax.axis_index("frag")
    last = jnp.full_like(frag, lax.axis_size("frag") - 1)
    meta = jnp.stack([core, chip, half, frag, last, place]).astype(jnp.int32)
    occ, fock, pair = occupied_pair_ladder[0], virtual_fock_block[0], pair_energy[0]
    near = factors[0]

    border = export_rows.shape[2]
    edge = shaped(border, row_count, virt)
    single = shaped(half_count, row_count, virt)
    single_low = shaped(half_count, row_count, virt, dtype=BF16)
    triple = shaped(3, half_count, row_count, virt)
    low_keep, low_send, *near_inputs = call(
        early_body,
        (
            single_low,
            single_low,
            shaped(*amps.shape[1:]),
            shaped(*amps.shape[1:]),
            shaped(*fock.shape),
            shaped(*virtual_orbital_energy.shape),
            shaped(*occ.shape),
            shaped(*pair_energy.shape),
            shaped(*energy_weight.shape, dtype=jnp.int32),
        ),
        (SMEM,) + (HBM,) * 7,
        meta,
        amps[0],
        exch[0],
        fock,
        virtual_orbital_energy,
        occ,
        pair_energy,
        energy_weight,
        scratch=(pltpu.SemaphoreType.DMA((7,)),),
    )
    amps, exch, fock, eps, occ, pair, weight = near_inputs
    keep, send, level, fock_low, own_weights, even_weights, odd_weights = call(
        open_body,
        (
            triple,
            triple,
            shaped(virt, virt),
            shaped(2, virt, virt, dtype=BF16),
            shaped(pairs, row_count, virt),
            edge,
            edge,
        ),
        (SMEM,) * 4 + (VMEM,) * 4,
        meta,
        occ,
        pair,
        weight,
        amps,
        exch,
        fock,
        eps,
    )
    lows = [low_keep]
    for value, step in ((low_send, 1), (low_keep, CROSS), (low_send, CROSS ^ 1)):
        lows.append(swap(value, step))
    far = swap(near, 1)
    came = swap(send, 1)
    came = swap(send, 1)
    far_keep = swap(keep[2], CROSS)
    far_came = swap(send[2], CROSS ^ 1)
    odd_came = odd_swap(odd_weights, False)
    own = shaped(half_count, both, virt)
    part, send = ladder(meta, fock_low, lows, near, far, keep, came)
    send, even_weights, odd_weights = lax.optimization_barrier((send, even_weights, odd_weights))
    part_came = swap(send, CROSS)
    even_came = even_swap(even_weights)
    odd_came = odd_swap(odd_weights, False)
    small = shaped(8, virt)
    low = shaped(half_count, virt, virt, dtype=BF16)
    amp, low, first, to_mate, keep_weights = call(
        middle_body,
        (own, low, small, shaped(half_count, both + row_count, virt), single),
        (SMEM, SMEM, SMEM) + (VMEM,) * 8,
        meta,
        pair,
        export_rows[0],
        part,
        part_came,
        level,
        keep,
        came,
        own_weights,
        even_came,
        odd_came,
        scratch=(pltpu.VMEM((pairs, row_count, virt), F32),),
    )
    from_mate = swap(to_mate, 1)
    send, part = ladder(meta, fock_low, (low,), near, far)
    part_came = swap(send, CROSS)
    base = call(
        hole_body,
        own,
        (SMEM, SMEM, SMEM) + (VMEM,) * 6,
        meta,
        occ,
        pair,
        amp,
        from_mate,
        keep,
        came,
        fock,
        level,
    )
    packed = shaped(half_count * row_count + 8, virt)
    last_keep, send, sums = call(
        last_body,
        (packed, packed, small),
        (SMEM, SMEM) + (VMEM,) * 8,
        meta,
        pair,
        part,
        part_came,
        level,
        base,
        amp,
        keep_weights,
        from_mate,
        first,
    )
    last_came = swap(send, 1)
    sum_cross = swap(sums, CROSS)
    sum_diag = swap(sums, CROSS ^ 1)
    rows = shaped(border * row_count, virt)
    whole, even_rows, odd_rows, sums = call(
        border_body,
        (shaped(pairs, row_count, virt), rows, rows, small),
        (SMEM, SMEM, VMEM, VMEM),
        meta,
        export_rows[0],
        last_keep,
        last_came,
    )
    sums = sums + (sum_cross + sum_diag)
    norm_squares = sums
    even_came = even_swap(jnp.concatenate([even_rows, sums], axis=0))
    sums = sums + even_came[border * row_count :]
    odd_came = odd_swap(jnp.concatenate([odd_rows, sums], axis=0), True)
    sums = sums + odd_came[border * row_count :]
    step = 4
    while step < lax.axis_size("frag"):
        sums = sums + wide_swap(sums, step)
        step *= 2
    new, norms = call(
        close_body,
        (shaped(row_count, pairs, virt), shaped(1, PASSES)),
        (SMEM, VMEM, VMEM, VMEM, VMEM),
        meta,
        whole,
        even_came,
        odd_came,
        norm_squares,
    )
    energy = -sums[0, 0] / (virt * virt)
    return new[None], norms, energy


def solution(mesh):
    placed = (
        P("frag", "blk", None, None),
        P("frag", "blk", None, None),
        P("frag", "blk", None, None),
        P("frag", None, None),
        P("frag", None, None),
        P("frag", None),
        P("frag", None),
        P("frag", None),
        P("frag", None, None),
    )

    return jax.shard_map(
        on_device,
        mesh=mesh,
        in_specs=placed,
        out_specs=(P("frag", "blk", None, None), P("frag", None), P()),
        check_vma=False,
    )
```

```python
import functools

import jax
import jax.numpy as jnp
from jax import lax
from jax.experimental import pallas as pl
from jax.experimental.pallas import tpu as pltpu
from jax.sharding import PartitionSpec as P

PASSES = 2
CROSS = 3
F32 = jnp.float32
BF16 = jnp.bfloat16

VMEM = pl.BlockSpec(memory_space=pltpu.VMEM)
SMEM = pl.BlockSpec(memory_space=pltpu.SMEM)
HBM = pl.BlockSpec(memory_space=pltpu.HBM)


def swap(value, step):
    count = lax.axis_size("blk")
    return lax.ppermute(value, "blk", [(at, at ^ step) for at in range(count)])


def even_swap(value):
    return wide_swap(value, 1)


def odd_swap(value, closed):
    count, width = lax.axis_size("frag"), lax.axis_size("blk")
    links = []
    for f in range(count):
        to = f + (1 if f % 2 else -1)
        to = to % count if closed or 0 <= to < count else f
        links += [(f * width + b, to * width + (b ^ 1)) for b in range(width)]
    return lax.ppermute(value, ("frag", "blk"), links)


def wide_swap(value, frag_step):
    count = lax.axis_size("blk")
    links = [
        (f * count + b, (f ^ frag_step) * count + (b ^ 1))
        for f in range(lax.axis_size("frag"))
        for b in range(count)
    ]
    return lax.ppermute(value, ("frag", "blk"), links)


def call(body, out_shape, specs, *args, scratch=(), limit=6, flops=0):
    args = [
        pltpu.with_memory_space_constraint(arg, pltpu.HBM) if spec is HBM else arg
        for spec, arg in zip(specs, args, strict=True)
    ]
    return pl.pallas_call(
        body,
        out_shape=out_shape,
        in_specs=specs,
        out_specs=jax.tree.map(lambda _: VMEM, out_shape),
        scratch_shapes=scratch,
        cost_estimate=pl.CostEstimate(flops=flops, bytes_accessed=0, transcendentals=0),
        compiler_params=pltpu.CompilerParams(vmem_limit_bytes=limit * 2**20),
    )(*args)


def shaped(*dims, dtype=F32):
    return jax.ShapeDtypeStruct(dims, dtype)


def times_fock(amp, fock):
    return lax.dot_general(
        amp,
        fock,
        (((1,), (1,)), ((), ())),
        precision=lax.Precision.HIGHEST,
        preferred_element_type=F32,
    )


def join(keep_first, keep, came):
    return jnp.where(
        keep_first,
        jnp.concatenate([keep, came], axis=0),
        jnp.concatenate([came, keep], axis=0),
    )


def early_body(
    meta,
    amps_in,
    exch_in,
    fock_in,
    eps_in,
    occ_in,
    pair_in,
    weight_in,
    low_keep,
    low_send,
    amps,
    exch,
    fock,
    eps,
    occ,
    pair,
    weight,
    sems,
):
    moves = (
        (amps_in, amps),
        (exch_in, exch),
        (fock_in, fock),
        (eps_in, eps),
        (occ_in, occ),
        (pair_in, pair),
        (weight_in, weight),
    )
    copies = [pltpu.make_async_copy(*move, sems.at[at]) for at, move in enumerate(moves)]
    for copy in copies:
        copy.start()
    copies[0].wait()
    half_count = amps.shape[1] // 2
    half = meta[2]
    for p in range(half_count):
        first = amps[:, p, :].astype(BF16)
        second = amps[:, half_count + p, :].astype(BF16)
        low_keep[p] = jnp.where(half == 0, first, second)
        low_send[p] = jnp.where(half == 0, second, first)
    for copy in copies[1:]:
        copy.wait()


def open_body(
    meta,
    occ,
    pair,
    weight,
    amps,
    exch,
    fock,
    eps,
    keep,
    send,
    level,
    fock_low,
    own,
):
    rows, pairs, _ = amps.shape
    half_count = pairs // 2
    border = (send.shape[0] - 3 * half_count) // 2
    even_at = 3 * half_count
    odd_at = even_at + border
    half = meta[2]
    at_start, at_end = meta[3] == 0, meta[3] == meta[4]
    is_even = meta[3] % 2 == 0
    wide = jnp.broadcast_to(eps[...], level.shape)
    level[...] = wide + wide.T
    levels = level[pl.ds(pl.multiple_of(meta[5] * rows, rows), rows), :]
    amp = [amps[:, p, :] for p in range(pairs)]
    turned = times_fock(jnp.concatenate(amp, axis=0), fock[...])
    for p in range(pairs):
        integral = exch[:, p, :]
        partial = integral + turned[p * rows : (p + 1) * rows]
        for r in range(pairs):
            partial = partial + occ[p, r] * amp[r]
        base = partial - (levels - pair[0, p]) * amp[p]
        at = p % half_count

        @pl.when(half == p // half_count)
        def _():
            keep[at], keep[half_count + at], keep[2 * half_count + at] = integral, base, partial

        @pl.when(half != p // half_count)
        def _():
            send[at], send[half_count + at], send[2 * half_count + at] = integral, base, partial

        weighted = (weight[0, p].astype(F32) * 0.5) * integral
        if p < border:
            send[jnp.where(is_even, odd_at, even_at) + p] = weighted
            weighted = jnp.where(at_start, weighted, 0.0)
        if p >= pairs - border:
            send[jnp.where(is_even, even_at, odd_at) + (p - (pairs - border))] = weighted
            weighted = jnp.where(at_end, weighted, 0.0)
        own[p] = weighted

    scaled = fock[...] * 0.5
    high = scaled.astype(BF16)
    fock_low[0] = high
    fock_low[1] = (scaled - high.astype(F32)).astype(BF16)


def hole_body(meta, occ, pair, amp, from_mate, keep, came, fock, level, base):
    half_count, rows, virt = amp.shape
    core, chip, half = meta[0], meta[1], meta[2]
    turned = times_fock(amp[...].reshape(half_count * rows, virt), fock[...])
    levels = level[pl.ds(pl.multiple_of(chip * rows, rows), rows), :]
    for p in range(half_count):
        at = half * half_count + p
        total = join(core == 0, keep[p], came[p])
        total = total + turned[p * rows : (p + 1) * rows] - (levels - pair[0, at]) * amp[p]
        for r in range(half_count):
            total = total + occ[at, half * half_count + r] * amp[r]
            total = total + occ[at, (1 - half) * half_count + r] * from_mate[r, :rows, :]
        base[p] = total


def ladder_body(meta, fock_low, *rest, group, count):
    lows, (source, far), rest = rest[:count], rest[count : count + 2], rest[count + 2 :]
    closing = count == 1
    if not closing:
        (keep, came), rest = rest[:2], rest[2:]
    outs, (near, gathered, turned, half_done, total, sem) = rest[:-6], rest[-6:]
    fetch = pltpu.make_async_copy(source, near, sem)
    fetch.start()
    half_count, rows, virt = lows[0].shape
    steps = far.shape[0] // group
    chip = meta[1]
    if count == 1:
        gathered = lows[0]
    else:
        for low, offset in zip(lows, (0, 1, CROSS, CROSS ^ 1), strict=True):
            at = jnp.bitwise_xor(meta[5], offset)
            gathered[:, pl.ds(pl.multiple_of(at * rows, rows), rows), :] = low[...]
    rows = virt // 2
    for p in range(half_count):
        turned[p * virt : (p + 1) * virt] = gathered[p].astype(F32).T.astype(BF16)

    contract_last = (((1,), (1,)), ((), ()))

    def first_half(slab, at, slot):
        for j in range(group // 2):
            two = slab[pl.ds(at * group + 2 * j, 2)].reshape(2 * virt, virt)
            part = lax.dot_general(
                turned[...], two, contract_last, preferred_element_type=F32
            ).astype(BF16)
            for p in range(half_count):
                for q in range(2):
                    half_done[
                        slot,
                        (2 * j + q) * virt : (2 * j + q + 1) * virt,
                        p * virt : (p + 1) * virt,
                    ] = part[p * virt : (p + 1) * virt, q * virt : (q + 1) * virt]

    def second_half(slab, at, slot):
        across = jnp.concatenate([slab[at * group + q] for q in range(group)], axis=1)
        total[...] += jnp.dot(across, half_done[slot], preferred_element_type=F32)

    fock_part = lax.dot_general(
        turned[...],
        fock_low[...].reshape(2 * virt, virt),
        contract_last,
        preferred_element_type=F32,
    )
    for p in range(half_count):
        block = fock_part[p * virt : (p + 1) * virt]
        total[:, p * virt : (p + 1) * virt] = block[:, :virt] + block[:, virt:]

    def sweep(slab, offset):
        def step(at, carry):
            second_half(slab, at - 1, (offset + at - 1) % 2)
            first_half(slab, at, (offset + at) % 2)
            return carry

        lax.fori_loop(1, steps, step, 0)

    first_half(far, 0, 0)
    sweep(far, 0)
    fetch.wait()
    second_half(far, steps - 1, (steps - 1) % 2)
    first_half(near, 0, steps % 2)
    sweep(near, steps)
    second_half(near, steps - 1, (2 * steps - 1) % 2)
    for p in range(half_count):
        block = total[:, p * virt : (p + 1) * virt].T
        top, bottom = block[:rows], block[rows:]
        if closing:
            send, kept = outs
            kept[p] = jnp.where(chip == 0, top, bottom)
            send[p] = jnp.where(chip == 0, bottom, top).astype(BF16)
        else:
            part, send = outs
            part[p] = block
            extra = join(meta[0] == 0, keep[2 * half_count + p], came[2 * half_count + p])
            send[p, :rows, :] = (top + jnp.where(chip == 0, extra, 0.0)).astype(BF16)
            send[p, rows:, :] = (bottom + jnp.where(chip == 0, 0.0, extra)).astype(BF16)


def ladder(meta, fock_low, lows, near, far, *own):
    half_count, _, virt = lows[0].shape
    rows = virt // 2
    aux = near.shape[0]
    group = max(g for g in range(2, 50, 2) if aux % g == 0)
    if own:
        out = (shaped(half_count, virt, virt), shaped(half_count, virt, virt, dtype=BF16))
    else:
        out = (shaped(half_count, rows, virt, dtype=BF16), shaped(half_count, rows, virt))
    return call(
        functools.partial(ladder_body, group=group, count=len(lows)),
        out,
        (SMEM,) + (VMEM,) * (1 + len(lows)) + (HBM, VMEM) + (VMEM,) * len(own),
        meta,
        fock_low,
        *lows,
        near,
        far,
        *own,
        scratch=(
            pltpu.VMEM((aux, virt, virt), BF16),
            pltpu.VMEM((half_count, virt, virt), BF16),
            pltpu.VMEM((half_count * virt, virt), BF16),
            pltpu.VMEM((2, group * virt, half_count * virt), BF16),
            pltpu.VMEM((virt, half_count * virt), F32),
            pltpu.SemaphoreType.DMA(()),
        ),
        limit=28,
        flops=8 * aux * half_count * virt**3,
    )


def fold_squares(residual):
    rows, virt = residual.shape
    return jnp.sum((residual * residual).reshape(rows // 8, 8, virt), axis=0)


def middle_body(
    meta,
    pair,
    picked,
    part,
    part_came,
    level,
    keep,
    came,
    own,
    even_came,
    odd_came,
    amp,
    low,
    squares,
    to_mate,
    keep_weights,
    weights,
):
    half_count, rows, _ = amp.shape
    core, chip, half = meta[0], meta[1], meta[2]
    mine = pl.ds(pl.multiple_of(chip * rows, rows), rows)
    other = pl.ds(pl.multiple_of((1 - chip) * rows, rows), rows)
    norm = jnp.zeros(squares.shape, F32)
    for p in range(half_count):
        shift_by = pair[0, half * half_count + p]
        lad = part[p, mine, :] + part_came[p, mine, :].astype(F32)
        fresh = (join(core == 0, keep[2 * half_count + p], came[2 * half_count + p]) + lad) / (level[mine, :] - shift_by)
        norm = norm + fold_squares(join(core == 0, keep[half_count + p], came[half_count + p]) + lad)
        amp[p] = fresh
        to_mate[p, :rows, :] = fresh
        low[p, mine, :] = fresh.astype(BF16)
        total = part[p, other, :] + part_came[p, other, :].astype(F32)
        low[p, other, :] = (total / (level[other, :] - shift_by)).astype(BF16)
    squares[...] = norm
    is_even, at_start, at_end = meta[3] % 2 == 0, meta[3] == 0, meta[3] == meta[4]
    weights[...] = own[...]
    for r in range(even_came.shape[0]):
        above = jnp.where(is_even, even_came[r], odd_came[r])
        below = jnp.where(is_even, odd_came[r], even_came[r])
        at = picked[0, r]
        weights[at] = weights[at] + jnp.where(at_end, 0.0, above)
        at = picked[1, r]
        weights[at] = weights[at] + jnp.where(at_start, 0.0, below)
    for p in range(half_count):
        keep_weights[p] = weights[half * half_count + p]
        to_mate[p, rows:, :] = weights[(1 - half) * half_count + p]


def last_body(
    meta, pair, part, came, level, base, amp, keep_weights, from_mate, first, packed, sums_out
):
    half_count, rows, virt = base.shape
    core, chip, half = meta[0], meta[1], meta[2]
    single = rows // 2
    levels = level[pl.ds(pl.multiple_of(chip * rows, rows), rows), :]
    norm = jnp.zeros(first.shape, F32)
    energy = jnp.zeros((single, virt), F32)
    for p in range(half_count):
        residual = base[p] + part[p] + came[p].astype(F32)
        norm = norm + fold_squares(residual)
        fresh = amp[p] + residual / (levels - pair[0, half * half_count + p])
        top, bottom = fresh[:single], fresh[single:]
        mine = jnp.where(core == 0, top, bottom)
        mate = jnp.where(core == 0, bottom, top)
        energy = energy + keep_weights[p] * mine + from_mate[p, rows:, :] * mate
        packed[p * single : (p + 1) * single, :] = mine
        packed[(half_count + p) * single : (half_count + p + 1) * single, :] = mate
    slot = lax.broadcasted_iota(jnp.int32, sums_out.shape, 0)
    sums = jnp.where(slot == 0, jnp.sum(energy), 0.0)
    sums = jnp.where(slot == 1, jnp.sum(first[...]), sums)
    sums = jnp.where(slot == 2, jnp.sum(norm), sums)
    packed[2 * half_count * single :, :] = sums
    sums_out[...] = sums


def border_body(meta, picked, packed, came, whole, even_rows, odd_rows, sums, mate):
    pairs, single, _ = whole.shape
    half_count = pairs // 2
    half = meta[2]
    mine_at = half * half_count
    mate_at = (1 - half) * half_count
    for p in range(half_count):
        first = slice(p * single, (p + 1) * single)
        second = slice((half_count + p) * single, (half_count + p + 1) * single)
        whole[mine_at + p] = packed[first, :]
        whole[mate_at + p] = came[second, :]
        mate[mine_at + p] = packed[second, :]
        mate[mate_at + p] = came[first, :]
    parity = meta[3] % 2
    for r in range(picked.shape[1]):
        even_rows[r * single : (r + 1) * single, :] = mate[picked[parity, r]]
        odd_rows[r * single : (r + 1) * single, :] = mate[picked[1 - parity, r]]
    sums[...] = packed[2 * half_count * single :, :] + came[2 * half_count * single :, :]


def close_body(meta, whole, even_came, odd_came, squares, new, norms):
    norms[...] = jnp.sqrt(jnp.concatenate([squares[1:2, 0:1], squares[2:3, 0:1]], axis=1))
    pairs, single, _ = whole.shape
    border = (even_came.shape[0] - 8) // single
    is_even, at_start, at_end = meta[3] % 2 == 0, meta[3] == 0, meta[3] == meta[4]
    for p in range(pairs):
        row = whole[p]
        if p < border:
            block = slice(p * single, (p + 1) * single)
            left = jnp.where(is_even, odd_came[block, :], even_came[block, :])
            row = jnp.where(at_start, row, left)
        if p >= pairs - border:
            at = p - (pairs - border)
            block = slice(at * single, (at + 1) * single)
            right = jnp.where(is_even, even_came[block, :], odd_came[block, :])
            row = jnp.where(at_end, row, right)
        new[:, p, :] = row


def on_device(
    amps,
    exch,
    factors,
    occupied_pair_ladder,
    virtual_fock_block,
    virtual_orbital_energy,
    pair_energy,
    energy_weight,
    export_rows,
):
    _, row_count, pairs, virt = amps.shape
    half_count = pairs // 2
    both = 2 * row_count
    place = lax.axis_index("blk")
    core, chip = place % 2, place // 2
    half = core ^ chip if CROSS == 3 else core
    frag = lax.axis_index("frag")
    last = jnp.full_like(frag, lax.axis_size("frag") - 1)
    meta = jnp.stack([core, chip, half, frag, last, place]).astype(jnp.int32)
    occ, fock, pair = occupied_pair_ladder[0], virtual_fock_block[0], pair_energy[0]
    near = factors[0]

    border = export_rows.shape[2]
    single = shaped(half_count, row_count, virt)
    single_low = shaped(half_count, row_count, virt, dtype=BF16)
    low_keep, low_send, *near_inputs = call(
        early_body,
        (
            single_low,
            single_low,
            shaped(*amps.shape[1:]),
            shaped(*amps.shape[1:]),
            shaped(*fock.shape),
            shaped(*virtual_orbital_energy.shape),
            shaped(*occ.shape),
            shaped(*pair_energy.shape),
            shaped(*energy_weight.shape, dtype=jnp.int32),
        ),
        (SMEM,) + (HBM,) * 7,
        meta,
        amps[0],
        exch[0],
        fock,
        virtual_orbital_energy,
        occ,
        pair_energy,
        energy_weight,
        scratch=(pltpu.SemaphoreType.DMA((7,)),),
    )
    amps, exch, fock, eps, occ, pair, weight = near_inputs
    keep, send, level, fock_low, own_weights = call(
        open_body,
        (
            shaped(3 * half_count, row_count, virt),
            shaped(3 * half_count + 2 * border, row_count, virt),
            shaped(virt, virt),
            shaped(2, virt, virt, dtype=BF16),
            shaped(pairs, row_count, virt),
        ),
        (SMEM,) * 4 + (VMEM,) * 4,
        meta,
        occ,
        pair,
        weight,
        amps,
        exch,
        fock,
        eps,
    )
    lows = [low_keep]
    for value, step in ((low_send, 1), (low_keep, CROSS), (low_send, CROSS ^ 1)):
        lows.append(swap(value, step))
    far = swap(near, 1)
    came = swap(send, 1)
    own = shaped(half_count, both, virt)
    part, send = ladder(meta, fock_low, lows, near, far, keep, came)
    even_at = 3 * half_count
    send, even_weights, odd_weights = lax.optimization_barrier(
        (send, came[even_at : even_at + border], came[even_at + border :])
    )
    part_came = swap(send, CROSS)
    even_came = even_swap(even_weights)
    odd_came = odd_swap(odd_weights, False)
    small = shaped(8, virt)
    low = shaped(half_count, virt, virt, dtype=BF16)
    amp, low, first, to_mate, keep_weights = call(
        middle_body,
        (own, low, small, shaped(half_count, both + row_count, virt), single),
        (SMEM, SMEM, SMEM) + (VMEM,) * 8,
        meta,
        pair,
        export_rows[0],
        part,
        part_came,
        level,
        keep,
        came,
        own_weights,
        even_came,
        odd_came,
        scratch=(pltpu.VMEM((pairs, row_count, virt), F32),),
    )
    from_mate = swap(to_mate, 1)
    send, part = ladder(meta, fock_low, (low,), near, far)
    part_came = swap(send, CROSS)
    base = call(
        hole_body,
        own,
        (SMEM, SMEM, SMEM) + (VMEM,) * 6,
        meta,
        occ,
        pair,
        amp,
        from_mate,
        keep,
        came,
        fock,
        level,
    )
    packed, sums = call(
        last_body,
        (shaped(pairs * row_count + 8, virt), small),
        (SMEM, SMEM) + (VMEM,) * 8,
        meta,
        pair,
        part,
        part_came,
        level,
        base,
        amp,
        keep_weights,
        from_mate,
        first,
    )
    last_came = swap(packed, 1)
    sum_cross = swap(sums, CROSS)
    sum_diag = swap(sums, CROSS ^ 1)
    rows = shaped(border * row_count, virt)
    whole, even_rows, odd_rows, sums = call(
        border_body,
        (shaped(pairs, row_count, virt), rows, rows, small),
        (SMEM, SMEM, VMEM, VMEM),
        meta,
        export_rows[0],
        packed,
        last_came,
        scratch=(pltpu.VMEM((pairs, row_count, virt), F32),),
    )
    sums = sums + (sum_cross + sum_diag)
    norm_squares = sums
    even_came = even_swap(jnp.concatenate([even_rows, sums], axis=0))
    sums = sums + even_came[border * row_count :]
    odd_came = odd_swap(jnp.concatenate([odd_rows, sums], axis=0), True)
    sums = sums + odd_came[border * row_count :]
    step = 4
    while step < lax.axis_size("frag"):
        sums = sums + wide_swap(sums, step)
        step *= 2
    new, norms = call(
        close_body,
        (shaped(row_count, pairs, virt), shaped(1, PASSES)),
        (SMEM, VMEM, VMEM, VMEM, VMEM),
        meta,
        whole,
        even_came,
        odd_came,
        norm_squares,
    )
    energy = -sums[0, 0] / (virt * virt)
    return new[None], norms, energy


def solution(mesh):
    placed = (
        P("frag", "blk", None, None),
        P("frag", "blk", None, None),
        P("frag", "blk", None, None),
        P("frag", None, None),
        P("frag", None, None),
        P("frag", None),
        P("frag", None),
        P("frag", None),
        P("frag", None, None),
    )

    return jax.shard_map(
        on_device,
        mesh=mesh,
        in_specs=placed,
        out_specs=(P("frag", "blk", None, None), P("frag", None), P()),
        check_vma=False,
    )
```

```python
import functools

import jax
import jax.numpy as jnp
from jax import lax
from jax.experimental import pallas as pl
from jax.experimental.pallas import tpu as pltpu
from jax.sharding import PartitionSpec as P

PASSES = 2
CROSS = 3
F32 = jnp.float32
BF16 = jnp.bfloat16

VMEM = pl.BlockSpec(memory_space=pltpu.VMEM)
SMEM = pl.BlockSpec(memory_space=pltpu.SMEM)
HBM = pl.BlockSpec(memory_space=pltpu.HBM)


def swap(value, step):
    count = lax.axis_size("blk")
    return lax.ppermute(value, "blk", [(at, at ^ step) for at in range(count)])


def even_swap(value):
    return wide_swap(value, 1)


def odd_swap(value, closed):
    count, width = lax.axis_size("frag"), lax.axis_size("blk")
    links = []
    for f in range(count):
        to = f + (1 if f % 2 else -1)
        to = to % count if closed or 0 <= to < count else f
        links += [(f * width + b, to * width + (b ^ 1)) for b in range(width)]
    return lax.ppermute(value, ("frag", "blk"), links)


def odd_far_swap(value):
    count, width = lax.axis_size("frag"), lax.axis_size("blk")
    links = []
    for f in range(count):
        source = f ^ 4
        source = (source + (1 if source % 2 else -1)) % count
        links += [(source * width + (b ^ 1), f * width + b) for b in range(width)]
    return lax.ppermute(value, ("frag", "blk"), links)


def wide_swap(value, frag_step, blk_step=1):
    count = lax.axis_size("blk")
    links = [
        (f * count + b, (f ^ frag_step) * count + (b ^ blk_step))
        for f in range(lax.axis_size("frag"))
        for b in range(count)
    ]
    return lax.ppermute(value, ("frag", "blk"), links)


def call(body, out_shape, specs, *args, scratch=(), limit=6, flops=0):
    args = [
        pltpu.with_memory_space_constraint(arg, pltpu.HBM) if spec is HBM else arg
        for spec, arg in zip(specs, args, strict=True)
    ]
    return pl.pallas_call(
        body,
        out_shape=out_shape,
        in_specs=specs,
        out_specs=jax.tree.map(lambda _: VMEM, out_shape),
        scratch_shapes=scratch,
        cost_estimate=pl.CostEstimate(flops=flops, bytes_accessed=0, transcendentals=0),
        compiler_params=pltpu.CompilerParams(vmem_limit_bytes=limit * 2**20),
    )(*args)


def shaped(*dims, dtype=F32):
    return jax.ShapeDtypeStruct(dims, dtype)


def times_fock(amp, fock):
    return lax.dot_general(
        amp,
        fock,
        (((1,), (1,)), ((), ())),
        precision=lax.Precision.HIGHEST,
        preferred_element_type=F32,
    )


def join(keep_first, keep, came):
    return jnp.where(
        keep_first,
        jnp.concatenate([keep, came], axis=0),
        jnp.concatenate([came, keep], axis=0),
    )


def early_body(
    meta,
    amps_in,
    exch_in,
    fock_in,
    eps_in,
    occ_in,
    pair_in,
    weight_in,
    low_keep,
    low_send,
    amps,
    exch,
    fock,
    eps,
    occ,
    pair,
    weight,
    sems,
):
    moves = (
        (amps_in, amps),
        (exch_in, exch),
        (fock_in, fock),
        (eps_in, eps),
        (occ_in, occ),
        (pair_in, pair),
        (weight_in, weight),
    )
    copies = [pltpu.make_async_copy(*move, sems.at[at]) for at, move in enumerate(moves)]
    for copy in copies:
        copy.start()
    copies[0].wait()
    half_count = amps.shape[1] // 2
    half = meta[2]
    for p in range(half_count):
        first = amps[:, p, :].astype(BF16)
        second = amps[:, half_count + p, :].astype(BF16)
        low_keep[p] = jnp.where(half == 0, first, second)
        low_send[p] = jnp.where(half == 0, second, first)
    for copy in copies[1:]:
        copy.wait()


def open_body(
    meta,
    occ,
    pair,
    weight,
    amps,
    exch,
    fock,
    eps,
    keep,
    send,
    level,
    fock_low,
    own,
):
    rows, pairs, _ = amps.shape
    half_count = pairs // 2
    border = (send.shape[0] - 3 * half_count) // 2
    even_at = 3 * half_count
    odd_at = even_at + border
    half = meta[2]
    at_start, at_end = meta[3] == 0, meta[3] == meta[4]
    is_even = meta[3] % 2 == 0
    wide = jnp.broadcast_to(eps[...], level.shape)
    level[...] = wide + wide.T
    levels = level[pl.ds(pl.multiple_of(meta[5] * rows, rows), rows), :]
    amp = [amps[:, p, :] for p in range(pairs)]
    turned = times_fock(jnp.concatenate(amp, axis=0), fock[...])
    for p in range(pairs):
        integral = exch[:, p, :]
        partial = integral + turned[p * rows : (p + 1) * rows]
        for r in range(pairs):
            partial = partial + occ[p, r] * amp[r]
        base = partial - (levels - pair[0, p]) * amp[p]
        at = p % half_count

        @pl.when(half == p // half_count)
        def _():
            keep[at], keep[half_count + at], keep[2 * half_count + at] = integral, base, partial

        @pl.when(half != p // half_count)
        def _():
            send[at], send[half_count + at], send[2 * half_count + at] = integral, base, partial

        weighted = (weight[0, p].astype(F32) * 0.5) * integral
        if p < border:
            send[jnp.where(is_even, odd_at, even_at) + p] = weighted
            weighted = jnp.where(at_start, weighted, 0.0)
        if p >= pairs - border:
            send[jnp.where(is_even, even_at, odd_at) + (p - (pairs - border))] = weighted
            weighted = jnp.where(at_end, weighted, 0.0)
        own[p] = weighted

    scaled = fock[...] * 0.5
    high = scaled.astype(BF16)
    fock_low[0] = high
    fock_low[1] = (scaled - high.astype(F32)).astype(BF16)


def hole_body(
    meta,
    occ,
    pair,
    picked,
    amp,
    from_mate,
    keep,
    came,
    fock,
    level,
    own,
    even_came,
    odd_came,
    base,
    keep_weights,
    mate_weights,
    weights,
):
    half_count, rows, virt = amp.shape
    core, chip, half = meta[0], meta[1], meta[2]
    turned = times_fock(amp[...].reshape(half_count * rows, virt), fock[...])
    levels = level[pl.ds(pl.multiple_of(chip * rows, rows), rows), :]
    for p in range(half_count):
        at = half * half_count + p
        total = join(core == 0, keep[p], came[p])
        total = total + turned[p * rows : (p + 1) * rows] - (levels - pair[0, at]) * amp[p]
        for r in range(half_count):
            total = total + occ[at, half * half_count + r] * amp[r]
            total = total + occ[at, (1 - half) * half_count + r] * from_mate[r]
        base[p] = total
    is_even, at_start, at_end = meta[3] % 2 == 0, meta[3] == 0, meta[3] == meta[4]
    weights[...] = own[...]
    for r in range(even_came.shape[0]):
        above = jnp.where(is_even, even_came[r], odd_came[r])
        below = jnp.where(is_even, odd_came[r], even_came[r])
        at = picked[0, r]
        weights[at] = weights[at] + jnp.where(at_end, 0.0, above)
        at = picked[1, r]
        weights[at] = weights[at] + jnp.where(at_start, 0.0, below)
    for p in range(half_count):
        keep_weights[p] = weights[half * half_count + p]
        mate_weights[p] = weights[(1 - half) * half_count + p]


def ladder_body(meta, fock_low, *rest, group, count):
    lows, (source, far), rest = rest[:count], rest[count : count + 2], rest[count + 2 :]
    closing = count == 1
    if not closing:
        (keep, came), rest = rest[:2], rest[2:]
    outs, (near, gathered, turned, half_done, total, sem) = rest[:-6], rest[-6:]
    fetch = pltpu.make_async_copy(source, near, sem)
    fetch.start()
    half_count, rows, virt = lows[0].shape
    steps = far.shape[0] // group
    chip = meta[1]
    if count == 1:
        gathered = lows[0]
    else:
        for low, offset in zip(lows, (0, 1, CROSS, CROSS ^ 1), strict=True):
            at = jnp.bitwise_xor(meta[5], offset)
            gathered[:, pl.ds(pl.multiple_of(at * rows, rows), rows), :] = low[...]
    rows = virt // 2
    for p in range(half_count):
        turned[p * virt : (p + 1) * virt] = gathered[p].astype(F32).T.astype(BF16)

    contract_last = (((1,), (1,)), ((), ()))

    def first_half(slab, at, slot):
        for j in range(group // 2):
            two = slab[pl.ds(at * group + 2 * j, 2)].reshape(2 * virt, virt)
            part = lax.dot_general(
                turned[...], two, contract_last, preferred_element_type=F32
            ).astype(BF16)
            for p in range(half_count):
                for q in range(2):
                    half_done[
                        slot,
                        (2 * j + q) * virt : (2 * j + q + 1) * virt,
                        p * virt : (p + 1) * virt,
                    ] = part[p * virt : (p + 1) * virt, q * virt : (q + 1) * virt]

    def second_half(slab, at, slot):
        across = jnp.concatenate([slab[at * group + q] for q in range(group)], axis=1)
        total[...] += jnp.dot(across, half_done[slot], preferred_element_type=F32)

    fock_part = lax.dot_general(
        turned[...],
        fock_low[...].reshape(2 * virt, virt),
        contract_last,
        preferred_element_type=F32,
    )
    for p in range(half_count):
        block = fock_part[p * virt : (p + 1) * virt]
        total[:, p * virt : (p + 1) * virt] = block[:, :virt] + block[:, virt:]

    def sweep(slab, offset):
        def step(at, carry):
            second_half(slab, at - 1, (offset + at - 1) % 2)
            first_half(slab, at, (offset + at) % 2)
            return carry

        lax.fori_loop(1, steps, step, 0)

    first_half(far, 0, 0)
    sweep(far, 0)
    fetch.wait()
    second_half(far, steps - 1, (steps - 1) % 2)
    first_half(near, 0, steps % 2)
    sweep(near, steps)
    second_half(near, steps - 1, (2 * steps - 1) % 2)
    for p in range(half_count):
        block = total[:, p * virt : (p + 1) * virt].T
        top, bottom = block[:rows], block[rows:]
        if closing:
            send, kept = outs
            kept[p] = jnp.where(chip == 0, top, bottom)
            send[p] = jnp.where(chip == 0, bottom, top).astype(BF16)
        else:
            part, send = outs
            part[p] = block
            extra = join(meta[0] == 0, keep[2 * half_count + p], came[2 * half_count + p])
            send[p, :rows, :] = (top + jnp.where(chip == 0, extra, 0.0)).astype(BF16)
            send[p, rows:, :] = (bottom + jnp.where(chip == 0, 0.0, extra)).astype(BF16)


def ladder(meta, fock_low, lows, near, far, *own):
    half_count, _, virt = lows[0].shape
    rows = virt // 2
    aux = near.shape[0]
    group = max(g for g in range(2, 50, 2) if aux % g == 0)
    if own:
        out = (shaped(half_count, virt, virt), shaped(half_count, virt, virt, dtype=BF16))
    else:
        out = (shaped(half_count, rows, virt, dtype=BF16), shaped(half_count, rows, virt))
    return call(
        functools.partial(ladder_body, group=group, count=len(lows)),
        out,
        (SMEM,) + (VMEM,) * (1 + len(lows)) + (HBM, VMEM) + (VMEM,) * len(own),
        meta,
        fock_low,
        *lows,
        near,
        far,
        *own,
        scratch=(
            pltpu.VMEM((aux, virt, virt), BF16),
            pltpu.VMEM((half_count, virt, virt), BF16),
            pltpu.VMEM((half_count * virt, virt), BF16),
            pltpu.VMEM((2, group * virt, half_count * virt), BF16),
            pltpu.VMEM((virt, half_count * virt), F32),
            pltpu.SemaphoreType.DMA(()),
        ),
        limit=28,
        flops=8 * aux * half_count * virt**3,
    )


def fold_squares(residual):
    rows, virt = residual.shape
    return jnp.sum((residual * residual).reshape(rows // 8, 8, virt), axis=0)


def middle_body(
    meta,
    pair,
    part,
    part_came,
    level,
    keep,
    came,
    amp,
    low,
    squares,
):
    half_count, rows, _ = amp.shape
    core, chip, half = meta[0], meta[1], meta[2]
    mine = pl.ds(pl.multiple_of(chip * rows, rows), rows)
    other = pl.ds(pl.multiple_of((1 - chip) * rows, rows), rows)
    norm = jnp.zeros(squares.shape, F32)
    for p in range(half_count):
        shift_by = pair[0, half * half_count + p]
        lad = part[p, mine, :] + part_came[p, mine, :].astype(F32)
        fresh = (join(core == 0, keep[2 * half_count + p], came[2 * half_count + p]) + lad) / (level[mine, :] - shift_by)
        norm = norm + fold_squares(join(core == 0, keep[half_count + p], came[half_count + p]) + lad)
        amp[p] = fresh
        low[p, mine, :] = fresh.astype(BF16)
        total = part[p, other, :] + part_came[p, other, :].astype(F32)
        low[p, other, :] = (total / (level[other, :] - shift_by)).astype(BF16)
    squares[...] = norm


def last_body(
    meta, pair, part, came, level, base, amp, keep_weights, from_mate, first, packed
):
    half_count, rows, virt = base.shape
    core, chip, half = meta[0], meta[1], meta[2]
    single = rows // 2
    levels = level[pl.ds(pl.multiple_of(chip * rows, rows), rows), :]
    norm = jnp.zeros(first.shape, F32)
    energy = jnp.zeros((single, virt), F32)
    for p in range(half_count):
        residual = base[p] + part[p] + came[p].astype(F32)
        norm = norm + fold_squares(residual)
        fresh = amp[p] + residual / (levels - pair[0, half * half_count + p])
        top, bottom = fresh[:single], fresh[single:]
        mine = jnp.where(core == 0, top, bottom)
        mate = jnp.where(core == 0, bottom, top)
        energy = energy + keep_weights[p] * mine + from_mate[p] * mate
        packed[p * single : (p + 1) * single, :] = mine
        packed[(half_count + p) * single : (half_count + p + 1) * single, :] = mate
    slot = lax.broadcasted_iota(jnp.int32, first.shape, 0)
    sums = jnp.where(slot == 0, jnp.sum(energy), 0.0)
    sums = jnp.where(slot == 1, jnp.sum(first[...]), sums)
    sums = jnp.where(slot == 2, jnp.sum(norm), sums)
    packed[2 * half_count * single :, :] = sums


def border_body(meta, picked, packed, came, whole, even_rows, odd_rows, sums, mate):
    pairs, single, _ = whole.shape
    half_count = pairs // 2
    half = meta[2]
    mine_at = half * half_count
    mate_at = (1 - half) * half_count
    for p in range(half_count):
        first = slice(p * single, (p + 1) * single)
        second = slice((half_count + p) * single, (half_count + p + 1) * single)
        whole[mine_at + p] = packed[first, :]
        whole[mate_at + p] = came[second, :]
        mate[mine_at + p] = packed[second, :]
        mate[mate_at + p] = came[first, :]
    parity = meta[3] % 2
    for r in range(picked.shape[1]):
        even_rows[r * single : (r + 1) * single, :] = mate[picked[parity, r]]
        odd_rows[r * single : (r + 1) * single, :] = mate[picked[1 - parity, r]]
    sums[...] = packed[2 * half_count * single :, :] + came[2 * half_count * single :, :]


def close_body(meta, whole, even_came, odd_came, squares, new, norms):
    norms[...] = jnp.sqrt(jnp.concatenate([squares[1:2, 0:1], squares[2:3, 0:1]], axis=1))
    pairs, single, _ = whole.shape
    border = (even_came.shape[0] - 8) // single
    is_even, at_start, at_end = meta[3] % 2 == 0, meta[3] == 0, meta[3] == meta[4]
    for p in range(pairs):
        row = whole[p]
        if p < border:
            block = slice(p * single, (p + 1) * single)
            left = jnp.where(is_even, odd_came[block, :], even_came[block, :])
            row = jnp.where(at_start, row, left)
        if p >= pairs - border:
            at = p - (pairs - border)
            block = slice(at * single, (at + 1) * single)
            right = jnp.where(is_even, even_came[block, :], odd_came[block, :])
            row = jnp.where(at_end, row, right)
        new[:, p, :] = row


def on_device(
    amps,
    exch,
    factors,
    occupied_pair_ladder,
    virtual_fock_block,
    virtual_orbital_energy,
    pair_energy,
    energy_weight,
    export_rows,
):
    _, row_count, pairs, virt = amps.shape
    half_count = pairs // 2
    both = 2 * row_count
    place = lax.axis_index("blk")
    core, chip = place % 2, place // 2
    half = core ^ chip if CROSS == 3 else core
    frag = lax.axis_index("frag")
    last = jnp.full_like(frag, lax.axis_size("frag") - 1)
    meta = jnp.stack([core, chip, half, frag, last, place]).astype(jnp.int32)
    occ, fock, pair = occupied_pair_ladder[0], virtual_fock_block[0], pair_energy[0]
    near = factors[0]

    border = export_rows.shape[2]
    single = shaped(half_count, row_count, virt)
    single_low = shaped(half_count, row_count, virt, dtype=BF16)
    low_keep, low_send, *near_inputs = call(
        early_body,
        (
            single_low,
            single_low,
            shaped(*amps.shape[1:]),
            shaped(*amps.shape[1:]),
            shaped(*fock.shape),
            shaped(*virtual_orbital_energy.shape),
            shaped(*occ.shape),
            shaped(*pair_energy.shape),
            shaped(*energy_weight.shape, dtype=jnp.int32),
        ),
        (SMEM,) + (HBM,) * 7,
        meta,
        amps[0],
        exch[0],
        fock,
        virtual_orbital_energy,
        occ,
        pair_energy,
        energy_weight,
        scratch=(pltpu.SemaphoreType.DMA((7,)),),
    )
    amps, exch, fock, eps, occ, pair, weight = near_inputs
    keep, send, level, fock_low, own_weights = call(
        open_body,
        (
            shaped(3 * half_count, row_count, virt),
            shaped(3 * half_count + 2 * border, row_count, virt),
            shaped(virt, virt),
            shaped(2, virt, virt, dtype=BF16),
            shaped(pairs, row_count, virt),
        ),
        (SMEM,) * 4 + (VMEM,) * 4,
        meta,
        occ,
        pair,
        weight,
        amps,
        exch,
        fock,
        eps,
    )
    lows = [low_keep]
    for value, step in ((low_send, 1), (low_keep, CROSS), (low_send, CROSS ^ 1)):
        lows.append(swap(value, step))
    far = swap(near, 1)
    came = swap(send, 1)
    own = shaped(half_count, both, virt)
    part, send = ladder(meta, fock_low, lows, near, far, keep, came)
    even_at = 3 * half_count
    send, even_weights, odd_weights = lax.optimization_barrier(
        (send, came[even_at : even_at + border], came[even_at + border :])
    )
    part_came = swap(send, CROSS)
    even_came = even_swap(even_weights)
    odd_came = odd_swap(odd_weights, False)
    small = shaped(8, virt)
    low = shaped(half_count, virt, virt, dtype=BF16)
    amp, low, first = call(
        middle_body,
        (own, low, small),
        (SMEM, SMEM) + (VMEM,) * 5,
        meta,
        pair,
        part,
        part_came,
        level,
        keep,
        came,
    )
    mate_amp = swap(amp, 1)
    send, part = ladder(meta, fock_low, (low,), near, far)
    part_came = swap(send, CROSS)
    base, keep_weights, mate_weights = call(
        hole_body,
        (own, single, single),
        (SMEM,) * 4 + (VMEM,) * 9,
        meta,
        occ,
        pair,
        export_rows[0],
        amp,
        mate_amp,
        keep,
        came,
        fock,
        level,
        own_weights,
        even_came,
        odd_came,
        scratch=(pltpu.VMEM((pairs, row_count, virt), F32),),
    )
    from_mate = swap(mate_weights, 1)
    packed = call(
        last_body,
        shaped(pairs * row_count + 8, virt),
        (SMEM, SMEM) + (VMEM,) * 8,
        meta,
        pair,
        part,
        part_came,
        level,
        base,
        amp,
        keep_weights,
        from_mate,
        first,
    )
    last_came = swap(packed, 1)
    rows = shaped(border * row_count, virt)
    whole, even_rows, odd_rows, sums = call(
        border_body,
        (shaped(pairs, row_count, virt), rows, rows, small),
        (SMEM, SMEM, VMEM, VMEM),
        meta,
        export_rows[0],
        packed,
        last_came,
        scratch=(pltpu.VMEM((pairs, row_count, virt), F32),),
    )
    tail = border * row_count
    even_came = even_swap(jnp.concatenate([even_rows, sums], axis=0))
    cross = swap(sums, CROSS)
    both_came = wide_swap(sums, 1, CROSS)
    norm_squares = sums + cross
    sums = norm_squares + (even_came[tail:] + both_came)
    odd_came = odd_swap(jnp.concatenate([odd_rows, sums], axis=0), True)
    if lax.axis_size("frag") > 4:
        far_came = wide_swap(sums, 4)
        next_came = odd_far_swap(sums)
        sums = (sums + odd_came[tail:]) + (far_came + next_came)
    else:
        sums = sums + odd_came[tail:]
    step = 8
    while step < lax.axis_size("frag"):
        sums = sums + wide_swap(sums, step)
        step *= 2
    new, norms = call(
        close_body,
        (shaped(row_count, pairs, virt), shaped(1, PASSES)),
        (SMEM, VMEM, VMEM, VMEM, VMEM),
        meta,
        whole,
        even_came,
        odd_came,
        norm_squares,
    )
    energy = -sums[0, 0] / (virt * virt)
    return new[None], norms, energy


def solution(mesh):
    placed = (
        P("frag", "blk", None, None),
        P("frag", "blk", None, None),
        P("frag", "blk", None, None),
        P("frag", None, None),
        P("frag", None, None),
        P("frag", None),
        P("frag", None),
        P("frag", None),
        P("frag", None, None),
    )

    return jax.shard_map(
        on_device,
        mesh=mesh,
        in_specs=placed,
        out_specs=(P("frag", "blk", None, None), P("frag", None), P()),
        check_vma=False,
    )
```

```python
import functools

import jax
import jax.numpy as jnp
from jax import lax
from jax.experimental import pallas as pl
from jax.experimental.pallas import tpu as pltpu
from jax.sharding import PartitionSpec as P

PASSES = 2
CROSS = 3
F32 = jnp.float32
BF16 = jnp.bfloat16

VMEM = pl.BlockSpec(memory_space=pltpu.VMEM)
SMEM = pl.BlockSpec(memory_space=pltpu.SMEM)
HBM = pl.BlockSpec(memory_space=pltpu.HBM)


def swap(value, step):
    count = lax.axis_size("blk")
    return lax.ppermute(value, "blk", [(at, at ^ step) for at in range(count)])


def even_swap(value):
    return wide_swap(value, 1)


def odd_swap(value, closed):
    count, width = lax.axis_size("frag"), lax.axis_size("blk")
    links = []
    for f in range(count):
        to = f + (1 if f % 2 else -1)
        to = to % count if closed or 0 <= to < count else f
        links += [(f * width + b, to * width + (b ^ 1)) for b in range(width)]
    return lax.ppermute(value, ("frag", "blk"), links)


def odd_far_swap(value):
    count, width = lax.axis_size("frag"), lax.axis_size("blk")
    links = []
    for f in range(count):
        source = f ^ 4
        source = (source + (1 if source % 2 else -1)) % count
        links += [(source * width + (b ^ 1), f * width + b) for b in range(width)]
    return lax.ppermute(value, ("frag", "blk"), links)


def wide_swap(value, frag_step, blk_step=1):
    count = lax.axis_size("blk")
    links = [
        (f * count + b, (f ^ frag_step) * count + (b ^ blk_step))
        for f in range(lax.axis_size("frag"))
        for b in range(count)
    ]
    return lax.ppermute(value, ("frag", "blk"), links)


def call(body, out_shape, specs, *args, scratch=(), limit=6, flops=0):
    args = [
        pltpu.with_memory_space_constraint(arg, pltpu.HBM) if spec is HBM else arg
        for spec, arg in zip(specs, args, strict=True)
    ]
    return pl.pallas_call(
        body,
        out_shape=out_shape,
        in_specs=specs,
        out_specs=jax.tree.map(lambda _: VMEM, out_shape),
        scratch_shapes=scratch,
        cost_estimate=pl.CostEstimate(flops=flops, bytes_accessed=0, transcendentals=0),
        compiler_params=pltpu.CompilerParams(vmem_limit_bytes=limit * 2**20),
    )(*args)


def shaped(*dims, dtype=F32):
    return jax.ShapeDtypeStruct(dims, dtype)


def times_fock(amp, fock):
    return lax.dot_general(
        amp,
        fock,
        (((1,), (1,)), ((), ())),
        precision=lax.Precision.HIGHEST,
        preferred_element_type=F32,
    )


def join(keep_first, keep, came):
    return jnp.where(
        keep_first,
        jnp.concatenate([keep, came], axis=0),
        jnp.concatenate([came, keep], axis=0),
    )


def early_body(
    meta,
    amps_in,
    exch_in,
    fock_in,
    eps_in,
    occ_in,
    pair_in,
    weight_in,
    low_keep,
    low_send,
    amps,
    exch,
    fock,
    eps,
    occ,
    pair,
    weight,
    sems,
):
    moves = (
        (amps_in, amps),
        (exch_in, exch),
        (fock_in, fock),
        (eps_in, eps),
        (occ_in, occ),
        (pair_in, pair),
        (weight_in, weight),
    )
    copies = [pltpu.make_async_copy(*move, sems.at[at]) for at, move in enumerate(moves)]
    for copy in copies:
        copy.start()
    copies[0].wait()
    half_count = amps.shape[1] // 2
    half = meta[2]
    for p in range(half_count):
        first = amps[:, p, :].astype(BF16)
        second = amps[:, half_count + p, :].astype(BF16)
        low_keep[p] = jnp.where(half == 0, first, second)
        low_send[p] = jnp.where(half == 0, second, first)
    for copy in copies[1:]:
        copy.wait()


def open_body(
    meta,
    occ,
    pair,
    weight,
    amps,
    exch,
    fock,
    eps,
    keep,
    send,
    level,
    fock_low,
    own,
):
    rows, pairs, _ = amps.shape
    half_count = pairs // 2
    border = (send.shape[0] - 3 * half_count) // 2
    even_at = 3 * half_count
    odd_at = even_at + border
    half = meta[2]
    at_start, at_end = meta[3] == 0, meta[3] == meta[4]
    is_even = meta[3] % 2 == 0
    wide = jnp.broadcast_to(eps[...], level.shape)
    level[...] = wide + wide.T
    levels = level[pl.ds(pl.multiple_of(meta[5] * rows, rows), rows), :]
    amp = [amps[:, p, :] for p in range(pairs)]
    turned = times_fock(jnp.concatenate(amp, axis=0), fock[...])
    for p in range(pairs):
        integral = exch[:, p, :]
        partial = integral + turned[p * rows : (p + 1) * rows]
        for r in range(pairs):
            partial = partial + occ[p, r] * amp[r]
        base = partial - (levels - pair[0, p]) * amp[p]
        at = p % half_count

        @pl.when(half == p // half_count)
        def _():
            keep[at], keep[half_count + at], keep[2 * half_count + at] = integral, base, partial

        @pl.when(half != p // half_count)
        def _():
            send[at], send[half_count + at], send[2 * half_count + at] = integral, base, partial

        weighted = (weight[0, p].astype(F32) * 0.5) * integral
        if p < border:
            send[jnp.where(is_even, odd_at, even_at) + p] = weighted
            weighted = jnp.where(at_start, weighted, 0.0)
        if p >= pairs - border:
            send[jnp.where(is_even, even_at, odd_at) + (p - (pairs - border))] = weighted
            weighted = jnp.where(at_end, weighted, 0.0)
        own[p] = weighted

    scaled = fock[...] * 0.5
    high = scaled.astype(BF16)
    fock_low[0] = high
    fock_low[1] = (scaled - high.astype(F32)).astype(BF16)


def hole_body(
    meta,
    occ,
    pair,
    picked,
    amp,
    from_mate,
    keep,
    came,
    fock,
    level,
    own,
    even_came,
    odd_came,
    base,
    keep_weights,
    mate_weights,
    weights,
):
    half_count, rows, virt = amp.shape
    core, chip, half = meta[0], meta[1], meta[2]
    turned = times_fock(amp[...].reshape(half_count * rows, virt), fock[...])
    levels = level[pl.ds(pl.multiple_of(chip * rows, rows), rows), :]
    for p in range(half_count):
        at = half * half_count + p
        total = join(core == 0, keep[p], came[p])
        total = total + turned[p * rows : (p + 1) * rows] - (levels - pair[0, at]) * amp[p]
        for r in range(half_count):
            total = total + occ[at, half * half_count + r] * amp[r]
            total = total + occ[at, (1 - half) * half_count + r] * from_mate[r]
        base[p] = total
    is_even, at_start, at_end = meta[3] % 2 == 0, meta[3] == 0, meta[3] == meta[4]
    weights[...] = own[...]
    for r in range(even_came.shape[0]):
        above = jnp.where(is_even, even_came[r], odd_came[r])
        below = jnp.where(is_even, odd_came[r], even_came[r])
        at = picked[0, r]
        weights[at] = weights[at] + jnp.where(at_end, 0.0, above)
        at = picked[1, r]
        weights[at] = weights[at] + jnp.where(at_start, 0.0, below)
    for p in range(half_count):
        keep_weights[p] = weights[half * half_count + p]
        mate_weights[p] = weights[(1 - half) * half_count + p]


def ladder_body(meta, fock_low, *rest, group, count):
    lows, (source, far), rest = rest[:count], rest[count : count + 2], rest[count + 2 :]
    closing = count == 1
    if not closing:
        (keep, came), rest = rest[:2], rest[2:]
    outs, (near, gathered, turned, half_done, total, sem) = rest[:-6], rest[-6:]
    fetch = pltpu.make_async_copy(source, near, sem)
    fetch.start()
    half_count, rows, virt = lows[0].shape
    steps = far.shape[0] // group
    chip = meta[1]
    if count == 1:
        gathered = lows[0]
    else:
        for low, offset in zip(lows, (0, 1, CROSS, CROSS ^ 1), strict=True):
            at = jnp.bitwise_xor(meta[5], offset)
            gathered[:, pl.ds(pl.multiple_of(at * rows, rows), rows), :] = low[...]
    rows = virt // 2
    for p in range(half_count):
        turned[p * virt : (p + 1) * virt] = gathered[p].astype(F32).T.astype(BF16)

    contract_last = (((1,), (1,)), ((), ()))

    def first_half(slab, at, slot):
        for j in range(group // 2):
            two = slab[pl.ds(at * group + 2 * j, 2)].reshape(2 * virt, virt)
            part = lax.dot_general(
                turned[...], two, contract_last, preferred_element_type=F32
            ).astype(BF16)
            for p in range(half_count):
                for q in range(2):
                    half_done[
                        slot,
                        (2 * j + q) * virt : (2 * j + q + 1) * virt,
                        p * virt : (p + 1) * virt,
                    ] = part[p * virt : (p + 1) * virt, q * virt : (q + 1) * virt]

    def second_half(slab, at, slot):
        across = jnp.concatenate([slab[at * group + q] for q in range(group)], axis=1)
        total[...] += jnp.dot(across, half_done[slot], preferred_element_type=F32)

    fock_part = lax.dot_general(
        turned[...],
        fock_low[...].reshape(2 * virt, virt),
        contract_last,
        preferred_element_type=F32,
    )
    for p in range(half_count):
        block = fock_part[p * virt : (p + 1) * virt]
        total[:, p * virt : (p + 1) * virt] = block[:, :virt] + block[:, virt:]

    def sweep(slab, offset):
        def step(at, carry):
            second_half(slab, at - 1, (offset + at - 1) % 2)
            first_half(slab, at, (offset + at) % 2)
            return carry

        lax.fori_loop(1, steps, step, 0)

    first_half(far, 0, 0)
    sweep(far, 0)
    fetch.wait()
    second_half(far, steps - 1, (steps - 1) % 2)
    first_half(near, 0, steps % 2)
    sweep(near, steps)
    second_half(near, steps - 1, (2 * steps - 1) % 2)
    for p in range(half_count):
        block = total[:, p * virt : (p + 1) * virt].T
        top, bottom = block[:rows], block[rows:]
        if closing:
            send, kept = outs
            kept[p] = jnp.where(chip == 0, top, bottom)
            send[p] = jnp.where(chip == 0, bottom, top).astype(BF16)
        else:
            part, send = outs
            part[p] = block
            extra = join(meta[0] == 0, keep[2 * half_count + p], came[2 * half_count + p])
            send[p, :rows, :] = (top + jnp.where(chip == 0, extra, 0.0)).astype(BF16)
            send[p, rows:, :] = (bottom + jnp.where(chip == 0, 0.0, extra)).astype(BF16)


def ladder(meta, fock_low, lows, near, far, *own):
    half_count, _, virt = lows[0].shape
    rows = virt // 2
    aux = near.shape[0]
    group = max(g for g in range(2, 98, 2) if aux % g == 0)
    if own:
        out = (shaped(half_count, virt, virt), shaped(half_count, virt, virt, dtype=BF16))
    else:
        out = (shaped(half_count, rows, virt, dtype=BF16), shaped(half_count, rows, virt))
    return call(
        functools.partial(ladder_body, group=group, count=len(lows)),
        out,
        (SMEM,) + (VMEM,) * (1 + len(lows)) + (HBM, VMEM) + (VMEM,) * len(own),
        meta,
        fock_low,
        *lows,
        near,
        far,
        *own,
        scratch=(
            pltpu.VMEM((aux, virt, virt), BF16),
            pltpu.VMEM((half_count, virt, virt), BF16),
            pltpu.VMEM((half_count * virt, virt), BF16),
            pltpu.VMEM((2, group * virt, half_count * virt), BF16),
            pltpu.VMEM((virt, half_count * virt), F32),
            pltpu.SemaphoreType.DMA(()),
        ),
        limit=42,
        flops=8 * aux * half_count * virt**3,
    )


def fold_squares(residual):
    rows, virt = residual.shape
    return jnp.sum((residual * residual).reshape(rows // 8, 8, virt), axis=0)


def middle_body(
    meta,
    pair,
    part,
    part_came,
    level,
    keep,
    came,
    amp,
    low,
    squares,
):
    half_count, rows, _ = amp.shape
    core, chip, half = meta[0], meta[1], meta[2]
    mine = pl.ds(pl.multiple_of(chip * rows, rows), rows)
    other = pl.ds(pl.multiple_of((1 - chip) * rows, rows), rows)
    norm = jnp.zeros(squares.shape, F32)
    for p in range(half_count):
        shift_by = pair[0, half * half_count + p]
        lad = part[p, mine, :] + part_came[p, mine, :].astype(F32)
        fresh = (join(core == 0, keep[2 * half_count + p], came[2 * half_count + p]) + lad) / (level[mine, :] - shift_by)
        norm = norm + fold_squares(join(core == 0, keep[half_count + p], came[half_count + p]) + lad)
        amp[p] = fresh
        low[p, mine, :] = fresh.astype(BF16)
        total = part[p, other, :] + part_came[p, other, :].astype(F32)
        low[p, other, :] = (total / (level[other, :] - shift_by)).astype(BF16)
    squares[...] = norm


def last_body(
    meta, pair, part, came, level, base, amp, keep_weights, from_mate, first, packed
):
    half_count, rows, virt = base.shape
    core, chip, half = meta[0], meta[1], meta[2]
    single = rows // 2
    levels = level[pl.ds(pl.multiple_of(chip * rows, rows), rows), :]
    norm = jnp.zeros(first.shape, F32)
    energy = jnp.zeros((single, virt), F32)
    for p in range(half_count):
        residual = base[p] + part[p] + came[p].astype(F32)
        norm = norm + fold_squares(residual)
        fresh = amp[p] + residual / (levels - pair[0, half * half_count + p])
        top, bottom = fresh[:single], fresh[single:]
        mine = jnp.where(core == 0, top, bottom)
        mate = jnp.where(core == 0, bottom, top)
        energy = energy + keep_weights[p] * mine + from_mate[p] * mate
        packed[p * single : (p + 1) * single, :] = mine
        packed[(half_count + p) * single : (half_count + p + 1) * single, :] = mate
    slot = lax.broadcasted_iota(jnp.int32, first.shape, 0)
    sums = jnp.where(slot == 0, jnp.sum(energy), 0.0)
    sums = jnp.where(slot == 1, jnp.sum(first[...]), sums)
    sums = jnp.where(slot == 2, jnp.sum(norm), sums)
    packed[2 * half_count * single :, :] = sums


def border_body(meta, picked, packed, came, whole, even_rows, odd_rows, mate):
    pairs, single, _ = whole.shape
    half_count = pairs // 2
    half = meta[2]
    mine_at = half * half_count
    mate_at = (1 - half) * half_count
    for p in range(half_count):
        first = slice(p * single, (p + 1) * single)
        second = slice((half_count + p) * single, (half_count + p + 1) * single)
        whole[mine_at + p] = packed[first, :]
        whole[mate_at + p] = came[second, :]
        mate[mine_at + p] = packed[second, :]
        mate[mate_at + p] = came[first, :]
    parity = meta[3] % 2
    for r in range(picked.shape[1]):
        even_rows[r * single : (r + 1) * single, :] = mate[picked[parity, r]]
        odd_rows[r * single : (r + 1) * single, :] = mate[picked[1 - parity, r]]


def close_body(meta, whole, even_came, odd_came, squares, new, norms):
    norms[...] = jnp.sqrt(jnp.concatenate([squares[1:2, 0:1], squares[2:3, 0:1]], axis=1))
    pairs, single, _ = whole.shape
    border = (even_came.shape[0] - 8) // single
    is_even, at_start, at_end = meta[3] % 2 == 0, meta[3] == 0, meta[3] == meta[4]
    for p in range(pairs):
        row = whole[p]
        if p < border:
            block = slice(p * single, (p + 1) * single)
            left = jnp.where(is_even, odd_came[block, :], even_came[block, :])
            row = jnp.where(at_start, row, left)
        if p >= pairs - border:
            at = p - (pairs - border)
            block = slice(at * single, (at + 1) * single)
            right = jnp.where(is_even, even_came[block, :], odd_came[block, :])
            row = jnp.where(at_end, row, right)
        new[:, p, :] = row


def on_device(
    amps,
    exch,
    factors,
    occupied_pair_ladder,
    virtual_fock_block,
    virtual_orbital_energy,
    pair_energy,
    energy_weight,
    export_rows,
):
    _, row_count, pairs, virt = amps.shape
    half_count = pairs // 2
    both = 2 * row_count
    place = lax.axis_index("blk")
    core, chip = place % 2, place // 2
    half = core ^ chip if CROSS == 3 else core
    frag = lax.axis_index("frag")
    last = jnp.full_like(frag, lax.axis_size("frag") - 1)
    meta = jnp.stack([core, chip, half, frag, last, place]).astype(jnp.int32)
    occ, fock, pair = occupied_pair_ladder[0], virtual_fock_block[0], pair_energy[0]
    near = factors[0]

    border = export_rows.shape[2]
    single = shaped(half_count, row_count, virt)
    single_low = shaped(half_count, row_count, virt, dtype=BF16)
    low_keep, low_send, *near_inputs = call(
        early_body,
        (
            single_low,
            single_low,
            shaped(*amps.shape[1:]),
            shaped(*amps.shape[1:]),
            shaped(*fock.shape),
            shaped(*virtual_orbital_energy.shape),
            shaped(*occ.shape),
            shaped(*pair_energy.shape),
            shaped(*energy_weight.shape, dtype=jnp.int32),
        ),
        (SMEM,) + (HBM,) * 7,
        meta,
        amps[0],
        exch[0],
        fock,
        virtual_orbital_energy,
        occ,
        pair_energy,
        energy_weight,
        scratch=(pltpu.SemaphoreType.DMA((7,)),),
    )
    amps, exch, fock, eps, occ, pair, weight = near_inputs
    keep, send, level, fock_low, own_weights = call(
        open_body,
        (
            shaped(3 * half_count, row_count, virt),
            shaped(3 * half_count + 2 * border, row_count, virt),
            shaped(virt, virt),
            shaped(2, virt, virt, dtype=BF16),
            shaped(pairs, row_count, virt),
        ),
        (SMEM,) * 4 + (VMEM,) * 4,
        meta,
        occ,
        pair,
        weight,
        amps,
        exch,
        fock,
        eps,
    )
    lows = [low_keep]
    for value, step in ((low_send, 1), (low_keep, CROSS), (low_send, CROSS ^ 1)):
        lows.append(swap(value, step))
    far = swap(near, 1)
    came = swap(send, 1)
    own = shaped(half_count, both, virt)
    part, send = ladder(meta, fock_low, lows, near, far, keep, came)
    even_at = 3 * half_count
    send, even_weights, odd_weights = lax.optimization_barrier(
        (send, came[even_at : even_at + border], came[even_at + border :])
    )
    part_came = swap(send, CROSS)
    even_came = even_swap(even_weights)
    odd_came = odd_swap(odd_weights, False)
    small = shaped(8, virt)
    low = shaped(half_count, virt, virt, dtype=BF16)
    amp, low, first = call(
        middle_body,
        (own, low, small),
        (SMEM, SMEM) + (VMEM,) * 5,
        meta,
        pair,
        part,
        part_came,
        level,
        keep,
        came,
    )
    mate_amp = swap(amp, 1)
    send, part = ladder(meta, fock_low, (low,), near, far)
    part_came = swap(send, CROSS)
    base, keep_weights, mate_weights = call(
        hole_body,
        (own, single, single),
        (SMEM,) * 4 + (VMEM,) * 9,
        meta,
        occ,
        pair,
        export_rows[0],
        amp,
        mate_amp,
        keep,
        came,
        fock,
        level,
        own_weights,
        even_came,
        odd_came,
        scratch=(pltpu.VMEM((pairs, row_count, virt), F32),),
    )
    from_mate = swap(mate_weights, 1)
    packed = call(
        last_body,
        shaped(pairs * row_count + 8, virt),
        (SMEM, SMEM) + (VMEM,) * 8,
        meta,
        pair,
        part,
        part_came,
        level,
        base,
        amp,
        keep_weights,
        from_mate,
        first,
    )
    last_came = swap(packed, 1)
    rows = shaped(border * row_count, virt)
    sums = packed[pairs * row_count :] + last_came[pairs * row_count :]
    cross = swap(sums, CROSS)
    both_came = wide_swap(sums, 1, CROSS)
    whole, even_rows, odd_rows = call(
        border_body,
        (shaped(pairs, row_count, virt), rows, rows),
        (SMEM, SMEM, VMEM, VMEM),
        meta,
        export_rows[0],
        packed,
        last_came,
        scratch=(pltpu.VMEM((pairs, row_count, virt), F32),),
    )
    tail = border * row_count
    even_came = even_swap(jnp.concatenate([even_rows, sums], axis=0))
    norm_squares = sums + cross
    sums = norm_squares + (even_came[tail:] + both_came)
    odd_came = odd_swap(jnp.concatenate([odd_rows, sums], axis=0), True)
    if lax.axis_size("frag") > 4:
        far_came = wide_swap(sums, 4)
        next_came = odd_far_swap(sums)
        sums = (sums + odd_came[tail:]) + (far_came + next_came)
    else:
        sums = sums + odd_came[tail:]
    step = 8
    while step < lax.axis_size("frag"):
        sums = sums + wide_swap(sums, step)
        step *= 2
    new, norms = call(
        close_body,
        (shaped(row_count, pairs, virt), shaped(1, PASSES)),
        (SMEM, VMEM, VMEM, VMEM, VMEM),
        meta,
        whole,
        even_came,
        odd_came,
        norm_squares,
    )
    energy = -sums[0, 0] / (virt * virt)
    return new[None], norms, energy


def solution(mesh):
    placed = (
        P("frag", "blk", None, None),
        P("frag", "blk", None, None),
        P("frag", "blk", None, None),
        P("frag", None, None),
        P("frag", None, None),
        P("frag", None),
        P("frag", None),
        P("frag", None),
        P("frag", None, None),
    )

    return jax.shard_map(
        on_device,
        mesh=mesh,
        in_specs=placed,
        out_specs=(P("frag", "blk", None, None), P("frag", None), P()),
        check_vma=False,
    )
```
